32 devices in a mesh: dp: 1 (over z), tp: 4 (over y), cp: 8 (over x, core).
Axes of the slice: x: 4, y: 4, z: 1, core: 2. Of those that a mesh axis runs over, the one named last changes fastest.
The devices are a block of a 4x4x8 slice.
Arguments:
- hidden: bfloat16 [8192, 1024], P(('dp', 'cp'))
- positions: int32 [8192], P(('dp', 'cp'))
- ln_gain: bfloat16 [1024], replicated
- w_q: bfloat16 [1024, 2048], P(None, 'tp')
- w_k: bfloat16 [1024, 1024], P(None, 'tp')
- w_v: bfloat16 [1024, 1024], P(None, 'tp')
- w_o: bfloat16 [2048, 1024], P('tp')
- w_gate: bfloat16 [1024, 3072], P(None, 'tp')
- w_up: bfloat16 [1024, 3072], P(None, 'tp')
- w_down: bfloat16 [3072, 1024], P('tp')
Outputs:
- output 1: bfloat16 [8192, 1024], P(('dp', 'cp'))
- output 2: bfloat16 [8192, 8, 128], P(('dp', 'cp'), 'tp')
- output 3: bfloat16 [8192, 8, 128], P(('dp', 'cp'), 'tp')
All inputs are finite; a program needn't handle non-finite values.
Results may differ from the reference program's by a relative error of at most 0.0126497.
Values are sent between devices in bfloat16 or wider.
A program may use at most 768 MiB of HBM per device.

```python
import jax
import jax.numpy as jnp
from jax import lax

D_MODEL = 1024
HEADS = 16
KV_HEADS = 8
FF_DIM = 3072
HEAD_DIM = 128
ROPE_BASE = 4000000
TOKENS = 8192
LN_EPS = 1e-5
Q_BLOCK = min(64, TOKENS)


def layer_norm(hidden, ln_gain):
    hidden_f = hidden.astype(jnp.float32)
    row_mean = jnp.mean(hidden_f, axis=-1, keepdims=True)
    centered = hidden_f - row_mean
    row_var = jnp.mean(centered * centered, axis=-1, keepdims=True)
    return (centered * lax.rsqrt(row_var + LN_EPS) * ln_gain.astype(jnp.float32)).astype(jnp.bfloat16)


def rotary(proj, positions):
    half_dim = HEAD_DIM // 2
    inv_freq = 1.0 / (ROPE_BASE ** (jnp.arange(0, HEAD_DIM, 2, dtype=jnp.float32) / HEAD_DIM))
    angles = positions.astype(jnp.float32)[:, None] * inv_freq[None, :]
    bcast_shape = (proj.shape[0],) + (1,) * (proj.ndim - 2) + (half_dim,)
    cosine = jnp.cos(angles).reshape(bcast_shape)
    sine_val = jnp.sin(angles).reshape(bcast_shape)
    paired = proj.astype(jnp.float32).reshape(proj.shape[:-1] + (half_dim, 2))
    even_part = paired[..., 0]
    odd_part = paired[..., 1]
    rotated = jnp.stack([even_part * cosine - odd_part * sine_val, odd_part * cosine + even_part * sine_val], axis=-1)
    return rotated.reshape(proj.shape).astype(jnp.bfloat16)


def setup_inputs(seed: int = 0, part: int = 0) -> dict:
    base_key = jax.random.key(seed)
    part_keys = jax.random.split(jax.random.fold_in(base_key, part), 2)
    weight_keys = jax.random.split(base_key, 8)
    q_width = HEADS * HEAD_DIM
    kv_width = KV_HEADS * HEAD_DIM
    d_scale = D_MODEL ** -0.5
    hidden = jax.random.normal(part_keys[0], (TOKENS, D_MODEL), jnp.float32)
    pos_steps = jax.random.randint(part_keys[1], (TOKENS,), 1, 3, dtype=jnp.int32)
    positions = (jnp.cumsum(pos_steps, dtype=jnp.int32) - pos_steps[0]).astype(jnp.int32)
    ln_gain = 1.0 + 0.3 * jax.random.normal(weight_keys[0], (D_MODEL,), jnp.float32)
    w_q = (1.5 * d_scale) * jax.random.normal(weight_keys[1], (D_MODEL, q_width), jnp.float32)
    w_k = (1.5 * d_scale) * jax.random.normal(weight_keys[2], (D_MODEL, kv_width), jnp.float32)
    w_v = d_scale * jax.random.normal(weight_keys[3], (D_MODEL, kv_width), jnp.float32)
    w_o = (2.0 * q_width ** -0.5) * jax.random.normal(weight_keys[4], (q_width, D_MODEL), jnp.float32)
    w_gate = d_scale * jax.random.normal(weight_keys[5], (D_MODEL, FF_DIM), jnp.float32)
    w_up = d_scale * jax.random.normal(weight_keys[6], (D_MODEL, FF_DIM), jnp.float32)
    w_down = (FF_DIM ** -0.5) * jax.random.normal(weight_keys[7], (FF_DIM, D_MODEL), jnp.float32)
    return {
        'hidden': hidden.astype(jnp.bfloat16),
        'positions': positions,
        'ln_gain': ln_gain.astype(jnp.bfloat16),
        'w_q': w_q.astype(jnp.bfloat16),
        'w_k': w_k.astype(jnp.bfloat16),
        'w_v': w_v.astype(jnp.bfloat16),
        'w_o': w_o.astype(jnp.bfloat16),
        'w_gate': w_gate.astype(jnp.bfloat16),
        'w_up': w_up.astype(jnp.bfloat16),
        'w_down': w_down.astype(jnp.bfloat16),
    }


def reference(hidden, positions, ln_gain, w_q, w_k, w_v, w_o, w_gate, w_up, w_down):
    group_size = HEADS // KV_HEADS
    normed = layer_norm(hidden, ln_gain)
    q_proj = jnp.dot(normed, w_q, preferred_element_type=jnp.float32).astype(jnp.bfloat16)
    k_proj = jnp.dot(normed, w_k, preferred_element_type=jnp.float32).astype(jnp.bfloat16)
    v_cache = jnp.dot(normed, w_v, preferred_element_type=jnp.float32).astype(jnp.bfloat16).reshape(TOKENS, KV_HEADS, HEAD_DIM)
    q_rot = rotary(q_proj.reshape(TOKENS, KV_HEADS, group_size, HEAD_DIM), positions)
    k_cache = rotary(k_proj.reshape(TOKENS, KV_HEADS, HEAD_DIM), positions)
    k_float = k_cache.astype(jnp.float32)
    v_float = v_cache.astype(jnp.float32)
    key_pos = jnp.arange(TOKENS)
    score_scale = HEAD_DIM ** -0.5
    q_blocks = q_rot.reshape(TOKENS // Q_BLOCK, Q_BLOCK, KV_HEADS, group_size, HEAD_DIM)

    def attend_block(block_args):
        block_id, q_block = block_args
        scores = jnp.einsum('qkgd,tkd->qkgt', q_block.astype(jnp.float32), k_float) * score_scale
        query_pos = block_id * Q_BLOCK + jnp.arange(Q_BLOCK)
        allowed = key_pos[None, :] <= query_pos[:, None]
        scores = jnp.where(allowed[:, None, None, :], scores, -jnp.inf)
        row_max = jnp.max(scores, axis=-1, keepdims=True)
        weights = jnp.exp(scores - row_max)
        row_sum = jnp.sum(weights, axis=-1, keepdims=True)
        probs = weights.astype(jnp.bfloat16).astype(jnp.float32)
        numer = jnp.einsum('qkgt,tkd->qkgd', probs, v_float)
        return (numer / row_sum).astype(jnp.bfloat16)

    attn = lax.map(attend_block, (jnp.arange(TOKENS // Q_BLOCK), q_blocks))
    attn_flat = attn.reshape(TOKENS, HEADS * HEAD_DIM)
    attn_out = jnp.dot(attn_flat, w_o, preferred_element_type=jnp.float32)
    gate_proj = jnp.dot(normed, w_gate, preferred_element_type=jnp.float32).astype(jnp.bfloat16)
    up_proj = jnp.dot(normed, w_up, preferred_element_type=jnp.float32).astype(jnp.bfloat16)
    mlp_act = (jax.nn.silu(gate_proj.astype(jnp.float32)) * up_proj.astype(jnp.float32)).astype(jnp.bfloat16)
    mlp_out = jnp.dot(mlp_act, w_down, preferred_element_type=jnp.float32)
    hidden_out = (hidden.astype(jnp.float32) + attn_out + mlp_out).astype(jnp.bfloat16)
    return (hidden_out, k_cache, v_cache)
```

```python
import functools

import jax
import jax.numpy as jnp
from jax import lax
from jax.experimental import pallas as pl
from jax.experimental.pallas import tpu as pltpu
from jax.sharding import PartitionSpec as P

HEAD_DIM = 128
ROPE_BASE = 4000000
LN_EPS = 1e-5
EXP2_SCALE = (HEAD_DIM ** -0.5) * 1.4426950408889634
MESH = pl.DeviceIdType.MESH
BF16 = jnp.bfloat16
F32 = jnp.float32


def rope_tables(positions):
    pair = jnp.repeat(jnp.arange(0, HEAD_DIM, 2, dtype=F32), 2)
    inv_freq = 1.0 / (ROPE_BASE ** (pair / HEAD_DIM))
    angles = positions.astype(F32)[:, None] * inv_freq[None, :]
    sign = jnp.where(jnp.arange(HEAD_DIM) % 2 == 0, -1.0, 1.0).astype(F32)
    return jnp.cos(angles), jnp.sin(angles) * sign[None, :]


def proj_kernel(hid_ref, cos_ref, sin_ref, gain_ref, wq_ref, wk_ref, wv_ref, h_ref, kvx_ref, kc_ref, vc_ref):
    x = hid_ref[...].astype(F32)
    mean = jnp.mean(x, axis=-1, keepdims=True)
    cent = x - mean
    var = jnp.mean(cent * cent, axis=-1, keepdims=True)
    h = (cent * lax.rsqrt(var + LN_EPS) * gain_ref[...].astype(F32)).astype(BF16)
    h_ref[...] = h
    cos, sin = cos_ref[...], sin_ref[...]
    even = lax.broadcasted_iota(jnp.int32, cos.shape, 1) % 2 == 0

    def rope(col):
        u = col.astype(BF16).astype(F32)
        swapped = jnp.where(even, pltpu.roll(u, HEAD_DIM - 1, 1), pltpu.roll(u, 1, 1))
        return (u * cos + swapped * sin).astype(BF16)

    q = jnp.dot(h, wq_ref[...], preferred_element_type=F32)
    k = jnp.dot(h, wk_ref[...], preferred_element_type=F32)
    v = jnp.dot(h, wv_ref[...], preferred_element_type=F32).astype(BF16)
    for g in range(2):
        kg = rope(k[:, g * HEAD_DIM:(g + 1) * HEAD_DIM])
        vg = v[:, g * HEAD_DIM:(g + 1) * HEAD_DIM]
        kvx_ref[g, 0] = kg
        kvx_ref[g, 1] = vg
        kc_ref[:, g * HEAD_DIM:(g + 1) * HEAD_DIM] = kg
        vc_ref[:, g * HEAD_DIM:(g + 1) * HEAD_DIM] = vg
        for j in range(2):
            lo = (2 * g + j) * HEAD_DIM
            kvx_ref[g, 2 + j] = rope(q[:, lo:lo + HEAD_DIM])


def project(hidden, cos, sin, gain, w_q, w_k, w_v):
    rows, width = hidden.shape
    tile = 256
    full = lambda a: pl.BlockSpec(a.shape, lambda i: (0, 0))
    return pl.pallas_call(
        proj_kernel,
        grid=(rows // tile,),
        in_specs=[
            pl.BlockSpec((tile, width), lambda i: (i, 0)),
            pl.BlockSpec((tile, HEAD_DIM), lambda i: (i, 0)),
            pl.BlockSpec((tile, HEAD_DIM), lambda i: (i, 0)),
            full(gain), full(w_q), full(w_k), full(w_v),
        ],
        out_specs=[
            pl.BlockSpec((tile, width), lambda i: (i, 0)),
            pl.BlockSpec((2, 4, tile, HEAD_DIM), lambda i: (0, 0, i, 0)),
            pl.BlockSpec((tile, 2 * HEAD_DIM), lambda i: (i, 0)),
            pl.BlockSpec((tile, 2 * HEAD_DIM), lambda i: (i, 0)),
        ],
        out_shape=[
            jax.ShapeDtypeStruct((rows, width), BF16),
            jax.ShapeDtypeStruct((2, 4, rows, HEAD_DIM), BF16),
            jax.ShapeDtypeStruct((rows, 2 * HEAD_DIM), BF16),
            jax.ShapeDtypeStruct((rows, 2 * HEAD_DIM), BF16),
        ],
        compiler_params=pltpu.CompilerParams(vmem_limit_bytes=40 << 20),
        name='proj',
    )(hidden, cos, sin, gain, w_q, w_k, w_v)


def layer_kernel(h_hbm, kvx_hbm, hid_hbm, wg_hbm, wu_hbm, wd_hbm, wo_hbm, out_hbm,
                 kvbuf, qbuf, acc, mbuf, lbuf, h, wg, wu, wd, wo, act, part, resid,
                 oown, osend, orecv, pbuf, rs1, sum2, rs2, xbuf,
                 load_sem, kvs_sem, kvr_sem, dds_sem, ddr_sem, ys_sem, yr_sem, out_sem):
    cp = lax.axis_index('cp')
    y = lax.axis_index('tp')
    x = cp // 2
    c = cp % 2
    partner = 2 * x + 1 - c
    right = ((x + 1) % 4) * 2 + c
    left = ((x + 3) % 4) * 2 + c
    y1 = y + 1 - 2 * (y % 2)
    y2 = 3 - y
    rows = h_hbm.shape[0]
    half_rows = rows // 2
    quarter = half_rows // 4
    sub = 256

    barrier = pltpu.get_barrier_semaphore()
    for dev in ({'cp': partner}, {'cp': right}, {'cp': left}, {'tp': y1}, {'tp': y2}):
        pl.semaphore_signal(barrier, inc=1, device_id=dev, device_id_type=MESH)

    own_kv = pltpu.make_async_copy(kvx_hbm.at[c, pl.ds(0, 2)], kvbuf.at[2 * x + c], load_sem.at[0])
    own_q = pltpu.make_async_copy(kvx_hbm.at[c, pl.ds(2, 2)], qbuf.at[c], load_sem.at[1])
    own_kv.start()
    own_q.start()
    loads = []
    for i, (src, dst) in enumerate(((h_hbm, h), (wg_hbm, wg), (wu_hbm, wu), (wd_hbm, wd), (wo_hbm, wo))):
        loads.append(pltpu.make_async_copy(src, dst, load_sem.at[2 + i]))
    for b in range(2):
        loads.append(pltpu.make_async_copy(
            hid_hbm.at[pl.ds(b * half_rows + y * quarter, quarter)], resid.at[b], load_sem.at[7 + b]))
    pl.semaphore_wait(barrier, 5)

    def remote(src, dst, ss, rsem, dev):
        return pltpu.make_async_remote_copy(src_ref=src, dst_ref=dst, send_sem=ss, recv_sem=rsem,
                                            device_id=dev, device_id_type=MESH)

    dd_kv = remote(kvx_hbm.at[1 - c, pl.ds(0, 2)], kvbuf.at[2 * x + c], dds_sem.at[0], ddr_sem.at[0], {'cp': partner})
    dd_q = remote(kvx_hbm.at[1 - c, pl.ds(2, 2)], qbuf.at[c], dds_sem.at[1], ddr_sem.at[1], {'cp': partner})
    dd_kv.start()
    dd_q.start()

    def kv_copy(ch, slot, dev):
        return remote(kvbuf.at[ch], kvbuf.at[ch], kvs_sem.at[slot], kvr_sem.at[ch], {'cp': dev})

    own_ch = 2 * x + c
    oth_ch = 2 * x + 1 - c
    own_kv.wait()

    @pl.when(x < 3)
    def _():
        kv_copy(own_ch, 0, right).start()

    @pl.when(x == 0)
    def _():
        kv_copy(own_ch, 1, left).start()

    for l in loads:
        l.start()
    loads[0].wait()
    loads[1].wait()
    loads[2].wait()
    loads[3].wait()

    def mlp(i, carry):
        rs = pl.ds(pl.multiple_of(i * sub, sub), sub)
        hh = h[rs, :]
        gate = jnp.dot(hh, wg[...], preferred_element_type=F32).astype(BF16).astype(F32)
        up = jnp.dot(hh, wu[...], preferred_element_type=F32).astype(BF16).astype(F32)
        a = (gate * (1.0 / (1.0 + jnp.exp(-gate))) * up).astype(BF16)
        part[rs, :] = jnp.dot(a, wd[...], preferred_element_type=F32)
        return carry

    lax.fori_loop(0, rows // sub, mlp, 0)

    remote(kvx_hbm.at[1 - c, pl.ds(0, 2)], kvbuf.at[oth_ch], dds_sem.at[0], ddr_sem.at[0], {'cp': partner}).wait_recv()
    remote(kvx_hbm.at[1 - c, pl.ds(2, 2)], qbuf.at[1 - c], dds_sem.at[1], ddr_sem.at[1], {'cp': partner}).wait_recv()
    own_q.wait()

    @pl.when(x < 3)
    def _():
        kv_copy(oth_ch, 2, right).start()

    @pl.when(x == 0)
    def _():
        kv_copy(oth_ch, 3, left).start()

    def lane_sum(p):
        s = p[:, :HEAD_DIM]
        for j in range(1, p.shape[1] // HEAD_DIM):
            s = s + p[:, j * HEAD_DIM:(j + 1) * HEAD_DIM]
        return s

    def qk(qv, kv):
        return lax.dot_general(qv, kv, (((1,), (1,)), ((), ())), preferred_element_type=F32)

    k0, k1, v0, v1 = (kvbuf.at[2 * x, 0], kvbuf.at[2 * x + 1, 0], kvbuf.at[2 * x, 1], kvbuf.at[2 * x + 1, 1])
    tri = (lax.broadcasted_iota(jnp.int32, (sub, sub), 1) <= lax.broadcasted_iota(jnp.int32, (sub, sub), 0))
    groups = rows // sub

    def diag_scores(r, g):
        half, off = r // groups, (r % groups) * sub
        qv = qbuf[half, g, pl.ds(off, sub), :]
        pieces = []
        if half == 1:
            pieces.append(qk(qv, k0[...]))
        kk = k0 if half == 0 else k1
        if off:
            pieces.append(qk(qv, kk[pl.ds(0, off), :]))
        pieces.append(jnp.where(tri, qk(qv, kk[pl.ds(off, sub), :]), -jnp.inf))
        return pieces[0] if len(pieces) == 1 else jnp.concatenate(pieces, axis=1)

    def diag_soft(r, g, s):
        half, off = r // groups, (r % groups) * sub
        rs = pl.ds(off, sub)
        mx = jnp.max(s, axis=1, keepdims=True)
        p = jnp.exp2((s - mx) * EXP2_SCALE)
        pb = p.astype(BF16)
        if half == 0:
            o = jnp.dot(pb, v0[pl.ds(0, off + sub), :], preferred_element_type=F32)
        else:
            o = jnp.dot(pb[:, :rows], v0[...], preferred_element_type=F32)
            o = o + jnp.dot(pb[:, rows:], v1[pl.ds(0, off + sub), :], preferred_element_type=F32)
        mbuf[g, half, rs, :] = jnp.broadcast_to(mx, (sub, HEAD_DIM))
        lbuf[g, half, rs, :] = lane_sum(p)
        acc[g, half, rs, :] = o

    items = [(r, g) for r in range(2 * groups) for g in range(2)]
    s_now = diag_scores(*items[0])
    for i, it in enumerate(items):
        s_next = diag_scores(*items[i + 1]) if i + 1 < len(items) else None
        diag_soft(*it, s_now)
        s_now = s_next

    for l in loads[4:]:
        l.wait()

    def attend(ch, b):
        kk, vv = kvbuf.at[ch, 0], kvbuf.at[ch, 1]
        its = [(g, half, pl.ds(pl.multiple_of(b * half_rows + j * sub, sub), sub))
               for half in range(2) for j in range(half_rows // sub) for g in range(2)]

        def scores(it):
            g, half, rs = it
            return qk(qbuf[half, g, rs, :], kk[...])

        s = scores(its[0])
        for i, it in enumerate(its):
            s_n = scores(its[i + 1]) if i + 1 < len(its) else None
            g, half, rs = it
            m_old = mbuf[g, half, rs, :]
            m_new = jnp.maximum(m_old, jnp.max(s, axis=1, keepdims=True))
            alpha = jnp.exp2((m_old - m_new) * EXP2_SCALE)
            p = jnp.exp2((s - m_new[:, :1]) * EXP2_SCALE)
            lbuf[g, half, rs, :] = lbuf[g, half, rs, :] * alpha + lane_sum(p)
            acc[g, half, rs, :] = acc[g, half, rs, :] * alpha + jnp.dot(
                p.astype(BF16), vv[...], preferred_element_type=F32)
            mbuf[g, half, rs, :] = m_new
            s = s_n

    first = (y1, y2)
    second = (y2, y1)

    def y_copy(src, dst, b, i, dev):
        return remote(src, dst, ys_sem.at[b, i], yr_sem.at[b, i], {'tp': dev})

    def rs1_copy(b, hf, slot):
        dev = first[hf]
        far = (3 - dev) if hf == 0 else (dev + 1 - 2 * (dev % 2))
        tile = dev if slot == 0 else far
        return y_copy(pbuf.at[b, tile, hf], rs1.at[b, hf, slot], b, 2 * hf + slot, dev)

    def rs2_copy(b, hf):
        return y_copy(sum2.at[b, hf], rs2.at[b, hf], b, 4 + hf, second[hf])

    def ag1_copy(b, hf):
        return y_copy(xbuf.at[b, y, hf], xbuf.at[b, y, hf], b, 6 + hf, second[hf])

    def ag1_wait(b, hf):
        t = second[hf]
        y_copy(xbuf.at[b, t, hf], xbuf.at[b, t, hf], b, 6 + hf, t).wait_recv()

    def ag2_copy(b, hf, slot):
        t = y if slot == 0 else second[hf]
        return y_copy(xbuf.at[b, t, hf], xbuf.at[b, t, hf], b, 8 + 2 * hf + slot, first[hf])

    def ag2_wait(b, hf, slot):
        dev = first[hf]
        far = (3 - dev) if hf == 0 else (dev + 1 - 2 * (dev % 2))
        t = dev if slot == 0 else far
        y_copy(xbuf.at[b, t, hf], xbuf.at[b, t, hf], b, 8 + 2 * hf + slot, dev).wait_recv()

    def o_copy(b):
        return remote(osend.at[b], orecv.at[b], dds_sem.at[2 + b], ddr_sem.at[2 + b], {'cp': partner})

    cols = (0, 512)

    def finish(b):
        base = b * half_rows

        def norm(half, j):
            rs = pl.ds(pl.multiple_of(base + j * quarter, quarter), quarter)
            out = []
            for g in range(2):
                den = jnp.sum(lbuf[g, half, rs, :], axis=1, keepdims=True)
                out.append((acc[g, half, rs, :] / den).astype(BF16))
            return jnp.concatenate(out, axis=1)

        def send_norm(j, carry):
            osend[b, pl.ds(pl.multiple_of(j * quarter, quarter), quarter), :] = norm(1 - c, j)
            return carry

        lax.fori_loop(0, 4, send_norm, 0)
        o_copy(b).start()
        wo_own = wo.at[pl.ds(pl.multiple_of(c * 2 * HEAD_DIM, 2 * HEAD_DIM), 2 * HEAD_DIM), :]
        wo_oth = wo.at[pl.ds(pl.multiple_of((1 - c) * 2 * HEAD_DIM, 2 * HEAD_DIM), 2 * HEAD_DIM), :]

        def own_part(j, carry):
            rs = pl.ds(pl.multiple_of(base + j * quarter, quarter), quarter)
            part[rs, :] = part[rs, :] + jnp.dot(norm(c, j), wo_own[...], preferred_element_type=F32)
            return carry

        lax.fori_loop(0, 4, own_part, 0)
        o_copy(b).wait_recv()

        def oth_part(j, carry):
            rs = pl.ds(pl.multiple_of(base + j * quarter, quarter), quarter)
            o = orecv[b, pl.ds(pl.multiple_of(j * quarter, quarter), quarter), :]
            tot = part[rs, :] + jnp.dot(o, wo_oth[...], preferred_element_type=F32)
            for hf in range(2):
                pbuf[b, j, hf] = tot[:, cols[hf]:cols[hf] + 512].astype(BF16)
            return carry

        lax.fori_loop(0, 4, oth_part, 0)
        for hf in range(2):
            for slot in range(2):
                rs1_copy(b, hf, 1 - slot).start()

    def step1(b):
        for hf in range(2):
            rs1_copy(b, hf, 1).wait_recv()
            other = second[hf]
            sum2[b, hf] = (pbuf[b, other, hf].astype(F32) + rs1[b, hf, 1].astype(F32)).astype(BF16)
            rs2_copy(b, hf).start()

    def step2(b):
        for hf in range(2):
            rs1_copy(b, hf, 0).wait_recv()
            rs2_copy(b, hf).wait_recv()
            tot = pbuf[b, y, hf].astype(F32) + rs1[b, hf, 0].astype(F32) + rs2[b, hf].astype(F32)
            tot = tot + resid[b, :, cols[hf]:cols[hf] + 512].astype(F32)
            xbuf[b, y, hf] = tot.astype(BF16)
            ag1_copy(b, hf).start()
            ag2_copy(b, hf, 0).start()

    def step3(b):
        for hf in range(2):
            ag1_wait(b, hf)
            ag2_copy(b, hf, 1).start()

    def out_copy(b, t, hf):
        return pltpu.make_async_copy(
            xbuf.at[b, t, hf],
            out_hbm.at[pl.ds(b * half_rows + t * quarter, quarter), pl.ds(cols[hf], 512)],
            out_sem.at[b, t, hf])

    def step4(b):
        for hf in range(2):
            for slot in range(2):
                ag2_wait(b, hf, slot)
        for t in range(4):
            for hf in range(2):
                out_copy(b, t, hf).start()

    n = 2 * x

    def chunk_of(s):
        first_half = s // 2
        par = s % 2
        near = 2 * (x - 1 - first_half) + (c + par - 2 * c * par)
        mix_half = c + first_half - 2 * c * first_half
        mixed = 4 - 4 * par + mix_half
        late = 2 + (c + par - 2 * c * par)
        three = jnp.where(s < 4, mixed, late)
        return jnp.where(x == 3, three, near)

    steps = 4 * x + 4 * (1 - (x + 3) // 4)

    def loop(t, carry):
        lead = steps - 4
        tail = t - lead
        in_tail = t >= lead
        s = jnp.where(in_tail, n - 2 + tail % 2, t // 2)
        b = jnp.where(in_tail, tail // 2, t % 2)

        @pl.when(x > 0)
        def _():
            ch = chunk_of(s)

            @pl.when(b == 0)
            def _():
                kv_copy(ch, 0, right).wait_recv()

                @pl.when(jnp.logical_and(x == 2, s < 2))
                def _():
                    kv_copy(ch, 1 + 2 * (s % 2), right).start()

                @pl.when(jnp.logical_and(x == 3, jnp.logical_and(s < 4, s % 2 == 1)))
                def _():
                    kv_copy(ch, s // 2, left).start()

            attend(ch, b)

        @pl.when(t == steps - 3)
        def _():
            finish(0)

        @pl.when(t == steps - 2)
        def _():
            step1(0)

        @pl.when(t == steps - 1)
        def _():
            step2(0)
        return carry

    lax.fori_loop(0, steps, loop, 0)
    finish(1)
    step3(0)
    step1(1)
    step4(0)
    step2(1)
    step3(1)
    step4(1)

    dd_kv.wait_send()
    dd_q.wait_send()

    @pl.when(x < 3)
    def _():
        kv_copy(own_ch, 0, right).wait_send()
        kv_copy(oth_ch, 2, right).wait_send()

    @pl.when(x == 0)
    def _():
        kv_copy(own_ch, 1, left).wait_send()
        kv_copy(oth_ch, 3, left).wait_send()

    @pl.when(x == 2)
    def _():
        kv_copy(own_ch, 1, right).wait_send()
        kv_copy(own_ch, 3, right).wait_send()

    @pl.when(x == 3)
    def _():
        kv_copy(own_ch, 0, left).wait_send()
        kv_copy(own_ch, 1, left).wait_send()

    for b in range(2):
        o_copy(b).wait_send()
        for hf in range(2):
            rs2_copy(b, hf).wait_send()
            ag1_copy(b, hf).wait_send()
            for slot in range(2):
                rs1_copy(b, hf, slot).wait_send()
                ag2_copy(b, hf, slot).wait_send()
        for t in range(4):
            for hf in range(2):
                out_copy(b, t, hf).wait()


def layer(h, kvx, hidden, w_gate, w_up, w_down, w_o):
    rows, width = h.shape
    ff = w_gate.shape[1]
    hr = rows // 2
    qr = hr // 4
    hw = width // 2
    anyspec = pl.BlockSpec(memory_space=pl.ANY)
    vm = pltpu.VMEM
    return pl.pallas_call(
        layer_kernel,
        in_specs=[anyspec] * 7,
        out_specs=anyspec,
        out_shape=jax.ShapeDtypeStruct((rows, width), BF16),
        scratch_shapes=[
            vm((8, 2, rows, HEAD_DIM), BF16),
            vm((2, 2, rows, HEAD_DIM), BF16),
            vm((2, 2, rows, HEAD_DIM), F32),
            vm((2, 2, rows, HEAD_DIM), F32),
            vm((2, 2, rows, HEAD_DIM), F32),
            vm((rows, width), BF16),
            vm((width, ff), BF16), vm((width, ff), BF16), vm((ff, width), BF16),
            vm(w_o.shape, BF16),
            vm((8, 128), BF16),
            vm((rows, width), F32),
            vm((2, qr, width), BF16),
            vm((8, 128), BF16),
            vm((2, hr, 2 * HEAD_DIM), BF16),
            vm((2, hr, 2 * HEAD_DIM), BF16),
            vm((2, 4, 2, qr, hw), BF16),
            vm((2, 2, 2, qr, hw), BF16),
            vm((2, 2, qr, hw), BF16),
            vm((2, 2, qr, hw), BF16),
            vm((2, 4, 2, qr, hw), BF16),
            pltpu.SemaphoreType.DMA((9,)),
            pltpu.SemaphoreType.DMA((4,)),
            pltpu.SemaphoreType.DMA((8,)),
            pltpu.SemaphoreType.DMA((4,)),
            pltpu.SemaphoreType.DMA((4,)),
            pltpu.SemaphoreType.DMA((2, 12)),
            pltpu.SemaphoreType.DMA((2, 12)),
            pltpu.SemaphoreType.DMA((2, 4, 2)),
        ],
        compiler_params=pltpu.CompilerParams(collective_id=0, has_side_effects=True, vmem_limit_bytes=60 << 20),
        name='layer',
    )(h, kvx, hidden, w_gate, w_up, w_down, w_o)


def solution(mesh):
    def local_layer(hidden, positions, ln_gain, w_q, w_k, w_v, w_o, w_gate, w_up, w_down):
        rows = hidden.shape[0]
        kv_local = w_k.shape[1] // HEAD_DIM
        cos, sin = rope_tables(positions)
        h, kvx, kc, vc = project(hidden, cos, sin, ln_gain[None, :], w_q, w_k, w_v)
        out = layer(h, kvx, hidden, w_gate, w_up, w_down, w_o)
        return out, kc.reshape(rows, kv_local, HEAD_DIM), vc.reshape(rows, kv_local, HEAD_DIM)

    row_spec = P(('dp', 'cp'), None)
    col_spec = P(None, 'tp')
    cache_spec = P(('dp', 'cp'), 'tp', None)
    in_specs = (row_spec, P(('dp', 'cp')), P(None), col_spec, col_spec, col_spec, P('tp', None), col_spec, col_spec, P('tp', None))
    return jax.shard_map(local_layer, mesh=mesh, in_specs=in_specs, out_specs=(row_spec, cache_spec, cache_spec), check_vma=False)
```

```python
import jax
import jax.numpy as jnp
import numpy as np
from jax import lax
from jax.experimental import pallas as pl
from jax.experimental.pallas import tpu as pltpu
from jax.sharding import PartitionSpec as P

HEAD_DIM = 128
ROPE_BASE = 4000000
LN_EPS = 1e-5
EXP2_SCALE = (HEAD_DIM ** -0.5) * 1.4426950408889634
MESH = pl.DeviceIdType.MESH
BF16 = jnp.bfloat16
F32 = jnp.float32


def sin_cos(angle):
    k = jnp.floor(angle * 0.6366197723675814 + 0.5)
    r = ((angle - k * 1.5703125) - k * 4.837512969970703125e-4) - k * 7.54978995489188216e-8
    z = r * r
    sn = r + r * z * (-1.6666654611e-1 + z * (8.3321608736e-3 - 1.9515295891e-4 * z))
    cs = 1.0 - 0.5 * z + z * z * (4.166664568298827e-2 + z * (-1.388731625493765e-3 + z * 2.443315711809948e-5))
    quad = k.astype(jnp.int32)
    odd = (quad & 1) == 1
    sin = jnp.where(odd, cs, sn)
    cos = jnp.where(odd, sn, cs)
    sin = jnp.where((quad & 2) == 2, -sin, sin)
    cos = jnp.where(((quad + 1) & 2) == 2, -cos, cos)
    return sin, cos


def layer_kernel(hid_hbm, pos_hbm, gain_hbm, freq_hbm, wq_hbm, wk_hbm, wv_hbm, wg_hbm, wu_hbm, wd_hbm, wo_hbm,
                 out_hbm, kc_hbm, vc_hbm,
                 kvbuf, qbuf, kvs, qs, acc, mbuf, lbuf, hid, h, pos, gain, freq, cost, sint,
                 wq, wk, wv, wg, wu, wd, wo, part, kc, vc,
                 osend, orecv, pbuf, rs1, sum2, rs2, xbuf,
                 load_sem, kvs_sem, kvr_sem, dds_sem, ddr_sem, ys_sem, yr_sem, out_sem):
    cp = lax.axis_index('cp')
    y = lax.axis_index('tp')
    x = cp // 2
    c = cp % 2
    partner = 2 * x + 1 - c
    right = ((x + 1) % 4) * 2 + c
    left = ((x + 3) % 4) * 2 + c
    y1 = y + 1 - 2 * (y % 2)
    y2 = 3 - y
    rows = hid_hbm.shape[0]
    sub = 256
    blocks = rows // sub
    quarter = sub // 4

    barrier = pltpu.get_barrier_semaphore()
    for dev in ({'cp': partner}, {'cp': right}, {'cp': left}, {'tp': y1}, {'tp': y2}):
        pl.semaphore_signal(barrier, inc=1, device_id=dev, device_id_type=MESH)

    pairs = ((hid_hbm, hid), (pos_hbm, pos), (gain_hbm, gain), (freq_hbm, freq), (wk_hbm, wk), (wv_hbm, wv), (wq_hbm, wq),
             (wg_hbm, wg), (wu_hbm, wu), (wd_hbm, wd), (wo_hbm, wo))
    loads = [pltpu.make_async_copy(src, dst, load_sem.at[i]) for i, (src, dst) in enumerate(pairs)]
    for i in (1, 3, 0, 2, 4, 5, 6):
        loads[i].start()

    def remote(src, dst, ss, rsem, dev):
        return pltpu.make_async_remote_copy(src_ref=src, dst_ref=dst, send_sem=ss, recv_sem=rsem,
                                            device_id=dev, device_id_type=MESH)

    def dd_kv(ch):
        return remote(kvs, kvbuf.at[ch], dds_sem.at[0], ddr_sem.at[0], {'cp': partner})

    def dd_q(half):
        return remote(qs, qbuf.at[half], dds_sem.at[1], ddr_sem.at[1], {'cp': partner})

    def kv_copy(ch, slot, dev):
        return remote(kvbuf.at[ch], kvbuf.at[ch], kvs_sem.at[slot], kvr_sem.at[ch], {'cp': dev})

    own_ch = 2 * x + c
    oth_ch = 2 * x + 1 - c

    loads[1].wait()
    loads[3].wait()
    lane = lax.broadcasted_iota(jnp.int32, (HEAD_DIM, HEAD_DIM), 1)
    for i in range(rows // HEAD_DIM):
        at = pl.ds(i * HEAD_DIM, HEAD_DIM)
        p = jnp.broadcast_to(pos[i:i + 1, :].astype(F32), (HEAD_DIM, HEAD_DIM)).T
        sn, cs = sin_cos(p * freq[...])
        cost[at, :] = cs
        sint[at, :] = jnp.where(lane % 2 == 0, -sn, sn)
    for i in (7, 8, 9, 10):
        loads[i].start()
    for i in (0, 2, 4, 5):
        loads[i].wait()

    even = lax.broadcasted_iota(jnp.int32, (sub, HEAD_DIM), 1) % 2 == 0
    gain_f = gain[...].astype(F32)
    gain_row = jnp.concatenate([gain_f[i:i + 1, :] for i in range(gain.shape[0])], axis=1)

    def rope(col, rs):
        u = col.astype(BF16).astype(F32)
        swapped = jnp.where(even, pltpu.roll(u, HEAD_DIM - 1, 1), pltpu.roll(u, 1, 1))
        return (u * cost[rs, :] + swapped * sint[rs, :]).astype(BF16)

    def project_kv(i, carry):
        rs = pl.ds(pl.multiple_of(i * sub, sub), sub)
        xx = hid[rs, :].astype(F32)
        cent = xx - jnp.mean(xx, axis=-1, keepdims=True)
        var = jnp.mean(cent * cent, axis=-1, keepdims=True)
        hh = (cent * lax.rsqrt(var + LN_EPS) * gain_row).astype(BF16)
        h[rs, :] = hh
        k = jnp.dot(hh, wk[...], preferred_element_type=F32)
        v = jnp.dot(hh, wv[...], preferred_element_type=F32).astype(BF16)
        vc[rs, :] = v
        for g in range(2):
            kc[rs, g * HEAD_DIM:(g + 1) * HEAD_DIM] = rope(k[:, g * HEAD_DIM:(g + 1) * HEAD_DIM], rs)

        def place(own, other):
            kvbuf[own_ch, 0, rs, :] = kc[rs, own * HEAD_DIM:(own + 1) * HEAD_DIM]
            kvbuf[own_ch, 1, rs, :] = vc[rs, own * HEAD_DIM:(own + 1) * HEAD_DIM]
            kvs[0, rs, :] = kc[rs, other * HEAD_DIM:(other + 1) * HEAD_DIM]
            kvs[1, rs, :] = vc[rs, other * HEAD_DIM:(other + 1) * HEAD_DIM]

        @pl.when(c == 0)
        def _():
            place(0, 1)

        @pl.when(c == 1)
        def _():
            place(1, 0)
        return carry

    with jax.named_scope('kvproj'):
        lax.fori_loop(0, rows // sub, project_kv, 0)
    pl.semaphore_wait(barrier, 5)
    dd_kv(own_ch).start()

    @pl.when(x < 3)
    def _():
        kv_copy(own_ch, 0, right).start()

    @pl.when(x == 0)
    def _():
        kv_copy(own_ch, 1, left).start()

    @pl.when(x == 1)
    def _():
        kv_copy(own_ch, 1, left).start()

    caches = (pltpu.make_async_copy(kc, kc_hbm, load_sem.at[11]), pltpu.make_async_copy(vc, vc_hbm, load_sem.at[12]))
    for cpy in caches:
        cpy.start()
    loads[6].wait()

    def project_q(i, carry):
        rs = pl.ds(pl.multiple_of(i * sub, sub), sub)
        q = jnp.dot(h[rs, :], wq[...], preferred_element_type=F32)
        for g in range(2):
            for j in range(2):
                lo = (2 * g + j) * HEAD_DIM
                qr = rope(q[:, lo:lo + HEAD_DIM], rs)

                @pl.when(c == g)
                def _():
                    qbuf[c, j, rs, :] = qr

                @pl.when(c != g)
                def _():
                    qs[j, rs, :] = qr
        return carry

    with jax.named_scope('qproj'):
        lax.fori_loop(0, rows // sub, project_q, 0)
    dd_q(c).start()
    dd_kv(oth_ch).wait_recv()

    @pl.when(x < 3)
    def _():
        kv_copy(oth_ch, 2, right).start()

    @pl.when(x == 0)
    def _():
        kv_copy(oth_ch, 3, left).start()

    loads[7].wait()
    loads[8].wait()
    loads[9].wait()

    def mlp(i, carry):
        rs = pl.ds(pl.multiple_of(i * sub, sub), sub)
        hh = h[rs, :]
        gate = jnp.dot(hh, wg[...], preferred_element_type=F32).astype(BF16).astype(F32)
        up = jnp.dot(hh, wu[...], preferred_element_type=F32).astype(BF16).astype(F32)
        a = (gate * (1.0 / (1.0 + jnp.exp(-gate))) * up).astype(BF16)
        part[rs, :] = jnp.dot(a, wd[...], preferred_element_type=F32)
        return carry

    with jax.named_scope('mlp'):
        lax.fori_loop(0, rows // sub, mlp, 0)

    dd_q(1 - c).wait_recv()

    def lane_sum(p):
        s = p[:, :HEAD_DIM]
        for j in range(1, p.shape[1] // HEAD_DIM):
            s = s + p[:, j * HEAD_DIM:(j + 1) * HEAD_DIM]
        return s

    def qk(qv, kv):
        return lax.dot_general(qv, kv, (((1,), (1,)), ((), ())), preferred_element_type=F32)

    k0, k1, v0, v1 = (kvbuf.at[2 * x, 0], kvbuf.at[2 * x + 1, 0], kvbuf.at[2 * x, 1], kvbuf.at[2 * x + 1, 1])
    tri = (lax.broadcasted_iota(jnp.int32, (sub, sub), 1) <= lax.broadcasted_iota(jnp.int32, (sub, sub), 0))
    groups = rows // sub

    def diag_scores(r, g):
        half, off = r // groups, (r % groups) * sub
        qv = qbuf[half, g, pl.ds(off, sub), :]
        pieces = []
        if half == 1:
            pieces.append(qk(qv, k0[...]))
        kk = k0 if half == 0 else k1
        if off:
            pieces.append(qk(qv, kk[pl.ds(0, off), :]))
        pieces.append(jnp.where(tri, qk(qv, kk[pl.ds(off, sub), :]), -jnp.inf))
        return pieces[0] if len(pieces) == 1 else jnp.concatenate(pieces, axis=1)

    def diag_soft(r, g, s):
        half, off = r // groups, (r % groups) * sub
        rs = pl.ds(off, sub)
        mx = jnp.max(s, axis=1, keepdims=True)
        p = jnp.exp2((s - mx) * EXP2_SCALE)
        pb = p.astype(BF16)
        if half == 0:
            o = jnp.dot(pb, v0[pl.ds(0, off + sub), :], preferred_element_type=F32)
        else:
            o = jnp.dot(pb[:, :rows], v0[...], preferred_element_type=F32)
            o = o + jnp.dot(pb[:, rows:], v1[pl.ds(0, off + sub), :], preferred_element_type=F32)
        mbuf[g, half, rs, :] = jnp.broadcast_to(mx, (sub, HEAD_DIM))
        lbuf[g, half, rs, :] = lane_sum(p)
        acc[g, half, rs, :] = o

    items = [(r, g) for r in range(2 * groups) for g in range(2)]
    own_block = jax.named_scope('diag')
    own_block.__enter__()
    s_now = diag_scores(*items[0])
    for i, it in enumerate(items):
        s_next = diag_scores(*items[i + 1]) if i + 1 < len(items) else None
        diag_soft(*it, s_now)
        s_now = s_next

    own_block.__exit__(None, None, None)
    loads[10].wait()

    @pl.when(x == 0)
    def _():
        kv_copy(2 + c, 0, right).wait_recv()
        kv_copy(2 + c, 4, left).start()

    def attend(chunks, its):
        def scores(it):
            g, half, rs = it
            qv = qbuf[half, g, rs, :]
            pieces = [qk(qv, kvbuf[ch, 0]) for ch in chunks]
            return pieces[0] if len(pieces) == 1 else jnp.concatenate(pieces, axis=1)

        s = scores(its[0])
        for i, it in enumerate(its):
            s_n = scores(its[i + 1]) if i + 1 < len(its) else None
            g, half, rs = it
            m_old = mbuf[g, half, rs, :]
            m_new = jnp.maximum(m_old, jnp.max(s, axis=1, keepdims=True))
            alpha = jnp.exp2((m_old - m_new) * EXP2_SCALE)
            p = jnp.exp2((s - m_new[:, :1]) * EXP2_SCALE)
            lbuf[g, half, rs, :] = lbuf[g, half, rs, :] * alpha + lane_sum(p)
            pb = p.astype(BF16)
            o = acc[g, half, rs, :] * alpha
            for i_ch, ch in enumerate(chunks):
                o = o + jnp.dot(pb[:, i_ch * rows:(i_ch + 1) * rows], kvbuf[ch, 1], preferred_element_type=F32)
            acc[g, half, rs, :] = o
            mbuf[g, half, rs, :] = m_new
            s = s_n

    def block_rows(b):
        return pl.ds(pl.multiple_of(b * sub, sub), sub)

    def attend_pair(ch, pair):
        attend((ch,), [(g, half, block_rows(2 * pair + j)) for half in range(2) for j in range(2) for g in range(2)])

    def attend_last(ch_a, ch_b, b):
        attend((ch_a, ch_b), [(g, half, block_rows(b)) for half in range(2) for g in range(2)])

    first = (y1, y2)
    second = (y2, y1)

    def y_copy(src, dst, b, i, dev):
        return remote(src, dst, ys_sem.at[b, i], yr_sem.at[b, i], {'tp': dev})

    def rs1_copy(b, hf, slot):
        dev = first[hf]
        far = (3 - dev) if hf == 0 else (dev + 1 - 2 * (dev % 2))
        tile = dev if slot == 0 else far
        return y_copy(pbuf.at[b, tile, hf], rs1.at[b, hf, slot], b, 2 * hf + slot, dev)

    def rs2_copy(b, hf):
        return y_copy(sum2.at[b, hf], rs2.at[b, hf], b, 4 + hf, second[hf])

    def ag1_copy(b, hf):
        return y_copy(xbuf.at[b, y, hf], xbuf.at[b, y, hf], b, 6 + hf, second[hf])

    def ag1_wait(b, hf):
        t = second[hf]
        y_copy(xbuf.at[b, t, hf], xbuf.at[b, t, hf], b, 6 + hf, t).wait_recv()

    def ag2_copy(b, hf, slot):
        t = y if slot == 0 else second[hf]
        return y_copy(xbuf.at[b, t, hf], xbuf.at[b, t, hf], b, 8 + 2 * hf + slot, first[hf])

    def ag2_wait(b, hf, slot):
        dev = first[hf]
        far = (3 - dev) if hf == 0 else (dev + 1 - 2 * (dev % 2))
        t = dev if slot == 0 else far
        y_copy(xbuf.at[b, t, hf], xbuf.at[b, t, hf], b, 8 + 2 * hf + slot, dev).wait_recv()

    def o_copy(b):
        return remote(osend.at[b], orecv.at[b], dds_sem.at[2 + b], ddr_sem.at[2 + b], {'cp': partner})

    cols = (0, 512)

    def finish(b):
        rs = block_rows(b)

        def norm(half):
            out = []
            for g in range(2):
                den = jnp.sum(lbuf[g, half, rs, :], axis=1, keepdims=True)
                out.append((acc[g, half, rs, :] / den).astype(BF16))
            return jnp.concatenate(out, axis=1)

        def wo_rows(group):
            return wo[pl.ds(pl.multiple_of(group * 2 * HEAD_DIM, 2 * HEAD_DIM), 2 * HEAD_DIM), :]

        osend[b] = norm(1 - c)
        o_copy(b).start()
        part[rs, :] = part[rs, :] + jnp.dot(norm(c), wo_rows(c), preferred_element_type=F32)
        o_copy(b).wait_recv()
        tot = (part[rs, :] + jnp.dot(orecv[b], wo_rows(1 - c), preferred_element_type=F32)).astype(BF16)
        for j in range(4):
            for hf in range(2):
                pbuf[b, j, hf] = tot[j * quarter:(j + 1) * quarter, cols[hf]:cols[hf] + 512]
        for slot in (1, 0):
            for hf in range(2):
                rs1_copy(b, hf, slot).start()

    def step1(b):
        for hf in range(2):
            rs1_copy(b, hf, 1).wait_recv()
            other = second[hf]
            sum2[b, hf] = (pbuf[b, other, hf].astype(F32) + rs1[b, hf, 1].astype(F32)).astype(BF16)
            rs2_copy(b, hf).start()

    def step2(b):
        own_rows = pl.ds(pl.multiple_of(b * sub + y * quarter, quarter), quarter)
        for hf in range(2):
            rs1_copy(b, hf, 0).wait_recv()
            rs2_copy(b, hf).wait_recv()
            tot = pbuf[b, y, hf].astype(F32) + rs1[b, hf, 0].astype(F32) + rs2[b, hf].astype(F32)
            tot = tot + hid[own_rows, cols[hf]:cols[hf] + 512].astype(F32)
            xbuf[b, y, hf] = tot.astype(BF16)
            ag1_copy(b, hf).start()
        for hf in range(2):
            ag2_copy(b, hf, 0).start()

    def step3(b):
        for hf in range(2):
            ag1_wait(b, hf)
            ag2_copy(b, hf, 1).start()

    def out_copy(b, t, hf):
        return pltpu.make_async_copy(
            xbuf.at[b, t, hf],
            out_hbm.at[pl.ds(b * sub + t * quarter, quarter), pl.ds(cols[hf], 512)],
            out_sem.at[b, t, hf])

    def step4(b):
        for hf in range(2):
            for slot in range(2):
                ag2_wait(b, hf, slot)
        for t in range(4):
            for hf in range(2):
                out_copy(b, t, hf).start()

    n = 2 * x

    def chunk_of(s):
        first_half = s // 2
        par = s % 2
        near = 2 * (x - 1 - first_half) + (c + par - 2 * c * par)
        mix_half = c + first_half - 2 * c * first_half
        mixed = 4 - 4 * par + mix_half
        late = 2 + (c + par - 2 * c * par)
        three = jnp.where(s < 4, mixed, late)
        return jnp.where(x == 3, three, near)

    three = x == 3
    lead = 4 * (x // 2) + 2 * (x // 3)
    ticks = lead + 8 + 2 * (x // 3)

    def pick(tau, near, far):
        b = jnp.int32(-1)
        for i in range(4):
            b = jnp.where(tau == jnp.where(three, far[i], near[i]), i, b)
        return jnp.maximum(b, 0), b >= 0

    def loop(t, carry):
        tau = t - lead
        gap = jnp.logical_and(three, jnp.logical_or(tau == 1, tau == 3))
        s3 = jnp.where(t == 0, 0, jnp.where(t == 1, 1, jnp.where(t == 2, 0, jnp.where(t == 3, 2, jnp.where(
            t == 4, 3, jnp.where(t == 5, 1, jnp.where(tau == 1, 2, 3)))))))
        pair3 = jnp.where(jnp.logical_or(t == 2, t >= 5), 1, 0)
        s = jnp.where(three, s3, t // 2)
        pair = jnp.where(three, pair3, t % 2)

        @pl.when(jnp.logical_and(x == 2, jnp.logical_and(tau < 0, t % 2 == 0)))
        def _():
            kv_copy(chunk_of(s), 0, right).wait_recv()

            @pl.when(t == 2)
            def _():
                kv_copy(chunk_of(1), 1, right).start()

        @pl.when(jnp.logical_and(three, jnp.logical_or(t == 0, t == 3)))
        def _():
            ch_b = chunk_of(s + 1)
            kv_copy(ch_b, 0, right).wait_recv()

            @pl.when(t == 0)
            def _():
                kv_copy(ch_b, 0, left).start()

            kv_copy(chunk_of(s), 0, right).wait_recv()

        @pl.when(jnp.logical_and(x > 0, tau == 0))
        def _():
            kv_copy(chunk_of(n - 2), 0, right).wait_recv()
            kv_copy(chunk_of(n - 1), 0, right).wait_recv()

            @pl.when(x == 1)
            def _():
                kv_copy(chunk_of(1), 3, right).start()

        @pl.when(jnp.logical_or(tau < 0, gap))
        def _():
            with jax.named_scope('att'):
                attend_pair(chunk_of(s), pair)

        b0, ok0 = pick(tau, (0, 1, 2, 3), (0, 2, 4, 5))

        @pl.when(jnp.logical_and(ok0, x > 0))
        def _():
            with jax.named_scope('last'):
                attend_last(chunk_of(n - 2), chunk_of(n - 1), b0)

        for fn, nm, near, far in ((step1, 's1', (2, 3, 4, 5), (2, 4, 6, 7)),
                                  (step2, 's2', (3, 4, 5, 6), (3, 5, 7, 8)),
                                  (step3, 's3', (4, 5, 6, 7), (4, 6, 8, 9))):
            bk, okk = pick(tau, near, far)

            @pl.when(okk)
            def _():
                with jax.named_scope(nm):
                    fn(bk)

        @pl.when(ok0)
        def _():
            with jax.named_scope('finish'):
                finish(b0)
        return carry

    lax.fori_loop(0, ticks, loop, 0)

    def last_step(b, carry):
        with jax.named_scope('s4'):
            step4(b)
        return carry

    lax.fori_loop(0, blocks, last_step, 0)

    dd_kv(own_ch).wait_send()
    dd_q(c).wait_send()
    for cpy in caches:
        cpy.wait()

    @pl.when(x < 3)
    def _():
        kv_copy(own_ch, 0, right).wait_send()
        kv_copy(own_ch, 1, right).wait_send()
        kv_copy(oth_ch, 2, right).wait_send()

    @pl.when(x == 0)
    def _():
        kv_copy(oth_ch, 3, left).wait_send()
        kv_copy(oth_ch, 4, left).wait_send()

    @pl.when(x == 1)
    def _():
        kv_copy(own_ch, 3, left).wait_send()

    @pl.when(x == 3)
    def _():
        kv_copy(own_ch, 0, left).wait_send()

    for b in range(blocks):
        o_copy(b).wait_send()
        for hf in range(2):
            rs2_copy(b, hf).wait_send()
            ag1_copy(b, hf).wait_send()
            for slot in range(2):
                rs1_copy(b, hf, slot).wait_send()
                ag2_copy(b, hf, slot).wait_send()
        for t in range(4):
            for hf in range(2):
                out_copy(b, t, hf).wait()


def layer(hidden, positions, gain, w_q, w_k, w_v, w_gate, w_up, w_down, w_o):
    rows, width = hidden.shape
    ff = w_gate.shape[1]
    hr = 256
    nb = rows // hr
    qr = hr // 4
    hw = width // 2
    freq = 1.0 / (ROPE_BASE ** (np.repeat(np.arange(0, HEAD_DIM, 2), 2) / HEAD_DIM))
    freq = jnp.asarray(freq[None, :], F32)
    anyspec = pl.BlockSpec(memory_space=pl.ANY)
    vm = pltpu.VMEM
    dma = pltpu.SemaphoreType.DMA
    return pl.pallas_call(
        layer_kernel,
        in_specs=[anyspec] * 11,
        out_specs=[anyspec] * 3,
        out_shape=[jax.ShapeDtypeStruct((rows, width), BF16),
                   jax.ShapeDtypeStruct((rows, w_k.shape[1]), BF16),
                   jax.ShapeDtypeStruct((rows, w_v.shape[1]), BF16)],
        scratch_shapes=[
            vm((8, 2, rows, HEAD_DIM), BF16),
            vm((2, 2, rows, HEAD_DIM), BF16),
            vm((2, rows, HEAD_DIM), BF16),
            vm((2, rows, HEAD_DIM), BF16),
            vm((2, 2, rows, HEAD_DIM), F32),
            vm((2, 2, rows, HEAD_DIM), F32),
            vm((2, 2, rows, HEAD_DIM), F32),
            vm((rows, width), BF16),
            vm((rows, width), BF16),
            vm((rows // HEAD_DIM, HEAD_DIM), jnp.int32),
            vm((width // HEAD_DIM, HEAD_DIM), BF16),
            vm((1, HEAD_DIM), F32),
            vm((rows, HEAD_DIM), F32),
            vm((rows, HEAD_DIM), F32),
            vm(w_q.shape, BF16), vm(w_k.shape, BF16), vm(w_v.shape, BF16),
            vm((width, ff), BF16), vm((width, ff), BF16), vm((ff, width), BF16),
            vm(w_o.shape, BF16),
            vm((rows, width), F32),
            vm((rows, w_k.shape[1]), BF16),
            vm((rows, w_v.shape[1]), BF16),
            vm((nb, hr, 2 * HEAD_DIM), BF16),
            vm((nb, hr, 2 * HEAD_DIM), BF16),
            vm((nb, 4, 2, qr, hw), BF16),
            vm((nb, 2, 2, qr, hw), BF16),
            vm((nb, 2, qr, hw), BF16),
            vm((nb, 2, qr, hw), BF16),
            vm((nb, 4, 2, qr, hw), BF16),
            dma((13,)), dma((5,)), dma((8,)), dma((2 + nb,)), dma((2 + nb,)), dma((nb, 12)), dma((nb, 12)), dma((nb, 4, 2)),
        ],
        compiler_params=pltpu.CompilerParams(collective_id=0, has_side_effects=True, vmem_limit_bytes=62 << 20),
        name='layer',
    )(hidden, positions.reshape(rows // HEAD_DIM, HEAD_DIM), gain.reshape(width // HEAD_DIM, HEAD_DIM), freq,
      w_q, w_k, w_v, w_gate, w_up, w_down, w_o)


def solution(mesh):
    def local_layer(hidden, positions, ln_gain, w_q, w_k, w_v, w_o, w_gate, w_up, w_down):
        rows = hidden.shape[0]
        kv_local = w_k.shape[1] // HEAD_DIM
        out, kc, vc = layer(hidden, positions, ln_gain, w_q, w_k, w_v, w_gate, w_up, w_down, w_o)
        return out, kc.reshape(rows, kv_local, HEAD_DIM), vc.reshape(rows, kv_local, HEAD_DIM)

    row_spec = P(('dp', 'cp'), None)
    col_spec = P(None, 'tp')
    cache_spec = P(('dp', 'cp'), 'tp', None)
    in_specs = (row_spec, P(('dp', 'cp')), P(None), col_spec, col_spec, col_spec, P('tp', None), col_spec, col_spec, P('tp', None))
    return jax.shard_map(local_layer, mesh=mesh, in_specs=in_specs, out_specs=(row_spec, cache_spec, cache_spec), check_vma=False)
```

```python
import jax
import jax.numpy as jnp
import numpy as np
from jax import lax
from jax.experimental import pallas as pl
from jax.experimental.pallas import tpu as pltpu
from jax.sharding import PartitionSpec as P

HEAD_DIM = 128
ROPE_BASE = 4000000
LN_EPS = 1e-5
EXP2_SCALE = (HEAD_DIM ** -0.5) * 1.4426950408889634
MESH = pl.DeviceIdType.MESH
BF16 = jnp.bfloat16
F32 = jnp.float32


def sin_cos(angle):
    k = jnp.floor(angle * 0.6366197723675814 + 0.5)
    r = ((angle - k * 1.5703125) - k * 4.837512969970703125e-4) - k * 7.54978995489188216e-8
    z = r * r
    sn = r + r * z * (-1.6666654611e-1 + z * (8.3321608736e-3 - 1.9515295891e-4 * z))
    cs = 1.0 - 0.5 * z + z * z * (4.166664568298827e-2 + z * (-1.388731625493765e-3 + z * 2.443315711809948e-5))
    quad = k.astype(jnp.int32)
    odd = (quad & 1) == 1
    sin = jnp.where(odd, cs, sn)
    cos = jnp.where(odd, sn, cs)
    sin = jnp.where((quad & 2) == 2, -sin, sin)
    cos = jnp.where(((quad + 1) & 2) == 2, -cos, cos)
    return sin, cos


def layer_kernel(hid_hbm, pos_hbm, gain_hbm, freq_hbm, wq_hbm, wk_hbm, wv_hbm, wg_hbm, wu_hbm, wd_hbm, wo_hbm,
                 out_hbm, kc_hbm, vc_hbm,
                 kvbuf, qbuf, kvs, qs, acc, mbuf, lbuf, hid, h, pos, gain, freq, cost, sint,
                 wq, wk, wv, wg, wu, wd, wo, wide, kc, vc,
                 mpart, mrs1, msum, mrs2, obuf, orecv, orelay, out,
                 load_sem, hid_sem, kvs_sem, kvr_sem, dds_sem, ddr_sem, es_sem, er_sem, ys_sem, yr_sem, out_sem):
    cp = lax.axis_index('cp')
    y = lax.axis_index('tp')
    x = cp // 2
    c = cp % 2
    partner = 2 * x + 1 - c
    right = ((x + 1) % 4) * 2 + c
    left = ((x + 3) % 4) * 2 + c
    y1 = y + 1 - 2 * (y % 2)
    y2 = 3 - y
    rows = hid_hbm.shape[0]
    sub = 256
    blocks = rows // sub
    quarter = sub // 4

    barrier = pltpu.get_barrier_semaphore()
    for dev in ({'cp': partner}, {'cp': right}, {'cp': left}, {'tp': y1}, {'tp': y2},
                {'tp': y1, 'cp': partner}, {'tp': y2, 'cp': partner}):
        pl.semaphore_signal(barrier, inc=1, device_id=dev, device_id_type=MESH)

    pairs = ((hid_hbm, hid), (pos_hbm, pos), (gain_hbm, gain), (freq_hbm, freq), (wk_hbm, wk), (wv_hbm, wv), (wq_hbm, wq),
             (wg_hbm, wg), (wu_hbm, wu), (wd_hbm, wd), (wo_hbm, wo.at[y]))
    loads = [pltpu.make_async_copy(src, dst, load_sem.at[i]) for i, (src, dst) in enumerate(pairs)]
    def hid_tile(i):
        rs = pl.ds(pl.multiple_of(i * sub, sub), sub)
        return pltpu.make_async_copy(hid_hbm.at[rs], hid.at[rs], hid_sem.at[i])

    loads[1].start()
    loads[3].start()
    hid_tile(0).start()
    for i in (2, 4, 5):
        loads[i].start()
    for i in range(1, blocks):
        hid_tile(i).start()
    for i in (6, 10):
        loads[i].start()

    def remote(src, dst, ss, rsem, dev):
        return pltpu.make_async_remote_copy(src_ref=src, dst_ref=dst, send_sem=ss, recv_sem=rsem,
                                            device_id=dev, device_id_type=MESH)

    def dd_kv(ch):
        return remote(kvs, kvbuf.at[ch], dds_sem.at[0], ddr_sem.at[0], {'cp': partner})

    def dd_q(half):
        return remote(qs, qbuf.at[half], dds_sem.at[1], ddr_sem.at[1], {'cp': partner})

    class KvCopy:
        def __init__(self, ch, slot, dev):
            self.parts = []
            for p in range(2):
                ref = kvbuf.at[ch, :, pl.ds(p * (rows // 2), rows // 2)]
                self.parts.append(remote(ref, ref, kvs_sem.at[slot, p], kvr_sem.at[ch, p], {'cp': dev}))

        def start(self):
            for part in self.parts:
                part.start()

        def wait_recv(self):
            for part in self.parts:
                part.wait_recv()

        def wait_send(self):
            for part in self.parts:
                part.wait_send()

    kv_copy = KvCopy

    first = (y1, y2)
    second = (y2, y1)
    far = 3 - y1

    def e_copy(src, dst, i, dev):
        return remote(src, dst, es_sem.at[i], er_sem.at[i], dev)

    w_half = 2 * HEAD_DIM

    def wo_rows(shard, lo, size):
        return wo.at[shard, pl.ds(pl.multiple_of(c * w_half + lo, HEAD_DIM), size)]

    def wo_direct(i, shard):
        ref = wo_rows(shard, 0, w_half)
        return e_copy(ref, ref, i, {'tp': first[i]})

    def wo_relay(hf, shard):
        ref = wo_rows(shard, hf * HEAD_DIM, HEAD_DIM)
        return e_copy(ref, ref, 2 + hf, {'tp': first[hf]})

    def wo_partner(i):
        ref = wo_rows((y1, y2, far)[i], 0, w_half)
        return e_copy(ref, ref, 4 + i, {'cp': partner})

    def mlp_rs1(hf, slot):
        dev = first[hf]
        beyond = (3 - dev) if hf == 0 else (dev + 1 - 2 * (dev % 2))
        tile = dev if slot == 0 else beyond
        return e_copy(mpart.at[tile, hf], mrs1.at[hf, slot], 7 + 2 * hf + slot, {'tp': dev})

    def mlp_rs2(hf):
        return e_copy(msum.at[hf], mrs2.at[hf], 11 + hf, {'tp': second[hf]})

    own_ch = 2 * x + c
    oth_ch = 2 * x + 1 - c

    loads[1].wait()
    loads[3].wait()
    lane = lax.broadcasted_iota(jnp.int32, (HEAD_DIM, HEAD_DIM), 1)
    for i in range(rows // HEAD_DIM):
        at = pl.ds(i * HEAD_DIM, HEAD_DIM)
        p = jnp.broadcast_to(pos[i:i + 1, :].astype(F32), (HEAD_DIM, HEAD_DIM)).T
        sn, cs = sin_cos(p * freq[...])
        cost[at, :] = cs
        sint[at, :] = jnp.where(lane % 2 == 0, -sn, sn)
    for i in (7, 8, 9):
        loads[i].start()
    for i in (2, 4, 5):
        loads[i].wait()

    even = lax.broadcasted_iota(jnp.int32, (sub, HEAD_DIM), 1) % 2 == 0
    gain_f = gain[...].astype(F32)
    gain_row = jnp.concatenate([gain_f[i:i + 1, :] for i in range(gain.shape[0])], axis=1)

    def rope(col, rs):
        u = col.astype(BF16).astype(F32)
        swapped = jnp.where(even, pltpu.roll(u, HEAD_DIM - 1, 1), pltpu.roll(u, 1, 1))
        return (u * cost[rs, :] + swapped * sint[rs, :]).astype(BF16)

    def project_kv(i, carry):
        rs = pl.ds(pl.multiple_of(i * sub, sub), sub)
        hid_tile(i).wait()
        xx = hid[rs, :].astype(F32)
        cent = xx - jnp.mean(xx, axis=-1, keepdims=True)
        var = jnp.mean(cent * cent, axis=-1, keepdims=True)
        hh = (cent * lax.rsqrt(var + LN_EPS) * gain_row).astype(BF16)
        h[rs, :] = hh
        k = jnp.dot(hh, wk[...], preferred_element_type=F32)
        v = jnp.dot(hh, wv[...], preferred_element_type=F32).astype(BF16)
        kk = [rope(k[:, g * HEAD_DIM:(g + 1) * HEAD_DIM], rs) for g in range(2)]
        vv = [v[:, g * HEAD_DIM:(g + 1) * HEAD_DIM] for g in range(2)]
        pair_rows = pl.ds(pl.multiple_of(i * 2 * sub, 2 * sub), 2 * sub)
        for slot, (vals, out) in enumerate(((kk, kc), (vv, vc))):
            for g in range(2):
                wide[slot, pl.ds(g, sub, 2), :] = vals[g].astype(F32)
            out[pair_rows, :] = wide[slot].astype(BF16)

        def place(own, other):
            kvbuf[own_ch, 0, rs, :] = kk[own]
            kvbuf[own_ch, 1, rs, :] = vv[own]
            kvs[0, rs, :] = kk[other]
            kvs[1, rs, :] = vv[other]

        @pl.when(c == 0)
        def _():
            place(0, 1)

        @pl.when(c == 1)
        def _():
            place(1, 0)
        return carry

    def send_own(p):
        @pl.when(x < 3)
        def _():
            kv_copy(own_ch, 0, right).parts[p].start()

        @pl.when(x < 2)
        def _():
            kv_copy(own_ch, 1, left).parts[p].start()

    with jax.named_scope('kvproj'):
        lax.fori_loop(0, blocks // 2, project_kv, 0)
    with jax.named_scope('bar'):
        pl.semaphore_wait(barrier, 7)
    send_own(0)
    with jax.named_scope('kvproj'):
        lax.fori_loop(blocks // 2, blocks, project_kv, 0)
    send_own(1)
    dd_kv(own_ch).start()

    loads[10].wait()
    for i in range(2):
        wo_direct(i, y).start()

    caches = (pltpu.make_async_copy(kc, kc_hbm, load_sem.at[11]), pltpu.make_async_copy(vc, vc_hbm, load_sem.at[12]))
    for cpy in caches:
        cpy.start()
    loads[6].wait()

    def project_q(i, carry):
        rs = pl.ds(pl.multiple_of(i * sub, sub), sub)
        q = jnp.dot(h[rs, :], wq[...], preferred_element_type=F32)
        for g in range(2):
            for j in range(2):
                lo = (2 * g + j) * HEAD_DIM
                qr = rope(q[:, lo:lo + HEAD_DIM], rs)

                @pl.when(c == g)
                def _():
                    qbuf[c, j, rs, :] = qr

                @pl.when(c != g)
                def _():
                    qs[j, rs, :] = qr
        return carry

    with jax.named_scope('qproj'):
        lax.fori_loop(0, rows // sub, project_q, 0)
    dd_q(c).start()
    dd_kv(oth_ch).wait_recv()

    @pl.when(x < 3)
    def _():
        kv_copy(oth_ch, 2, right).start()

    @pl.when(x == 0)
    def _():
        kv_copy(oth_ch, 3, left).start()

    loads[7].wait()
    loads[8].wait()
    loads[9].wait()

    cols = (0, 512)

    def mlp(i, carry):
        rs = pl.ds(pl.multiple_of(i * sub, sub), sub)
        hh = h[rs, :]
        gate = jnp.dot(hh, wg[...], preferred_element_type=F32).astype(BF16).astype(F32)
        up = jnp.dot(hh, wu[...], preferred_element_type=F32).astype(BF16).astype(F32)
        a = (gate * (1.0 / (1.0 + jnp.exp(-gate))) * up).astype(BF16)
        tot = jnp.dot(a, wd[...], preferred_element_type=F32).astype(BF16)
        for j in range(4):
            for hf in range(2):
                mpart[j, hf, i] = tot[j * quarter:(j + 1) * quarter, cols[hf]:cols[hf] + 512]
        return carry

    with jax.named_scope('mlp'):
        lax.fori_loop(0, rows // sub, mlp, 0)

    for slot in (1, 0):
        for hf in range(2):
            mlp_rs1(hf, slot).start()
    dd_q(1 - c).wait_recv()

    def lane_sum(p):
        s = p[:, :HEAD_DIM]
        for j in range(1, p.shape[1] // HEAD_DIM):
            s = s + p[:, j * HEAD_DIM:(j + 1) * HEAD_DIM]
        return s

    def qk(qv, kv):
        return lax.dot_general(qv, kv, (((1,), (1,)), ((), ())), preferred_element_type=F32)

    k0, k1, v0, v1 = (kvbuf.at[2 * x, 0], kvbuf.at[2 * x + 1, 0], kvbuf.at[2 * x, 1], kvbuf.at[2 * x + 1, 1])
    tri = (lax.broadcasted_iota(jnp.int32, (sub, sub), 1) <= lax.broadcasted_iota(jnp.int32, (sub, sub), 0))
    groups = rows // sub

    def diag_scores(r, g):
        half, off = r // groups, (r % groups) * sub
        qv = qbuf[half, g, pl.ds(off, sub), :]
        pieces = []
        if half == 1:
            pieces.append(qk(qv, k0[...]))
        kk = k0 if half == 0 else k1
        if off:
            pieces.append(qk(qv, kk[pl.ds(0, off), :]))
        pieces.append(jnp.where(tri, qk(qv, kk[pl.ds(off, sub), :]), -jnp.inf))
        return pieces[0] if len(pieces) == 1 else jnp.concatenate(pieces, axis=1)

    def diag_soft(r, g, s):
        half, off = r // groups, (r % groups) * sub
        rs = pl.ds(off, sub)
        mx = jnp.max(s, axis=1, keepdims=True)
        p = jnp.exp2((s - mx) * EXP2_SCALE)
        pb = p.astype(BF16)
        if half == 0:
            o = jnp.dot(pb, v0[pl.ds(0, off + sub), :], preferred_element_type=F32)
        else:
            o = jnp.dot(pb[:, :rows], v0[...], preferred_element_type=F32)
            o = o + jnp.dot(pb[:, rows:], v1[pl.ds(0, off + sub), :], preferred_element_type=F32)
        mbuf[g, half, rs, :] = jnp.broadcast_to(mx, (sub, HEAD_DIM))
        lbuf[g, half, rs, :] = lane_sum(p)
        acc[g, half, rs, :] = o

    items = [(r, g) for r in range(2 * groups) for g in range(2)]
    own_block = jax.named_scope('diag')
    own_block.__enter__()
    s_now = diag_scores(*items[0])
    for i, it in enumerate(items):
        s_next = diag_scores(*items[i + 1]) if i + 1 < len(items) else None
        diag_soft(*it, s_now)
        s_now = s_next

    own_block.__exit__(None, None, None)
    for hf in range(2):
        wo_direct(1 - hf, second[hf]).wait_recv()
        wo_relay(hf, second[hf]).start()

    @pl.when(x == 0)
    def _():
        kv_copy(2 + c, 0, right).wait_recv()
        kv_copy(2 + c, 4, left).start()

    def attend(chunks, its):
        def scores(it):
            g, half, rs = it
            qv = qbuf[half, g, rs, :]
            pieces = [qk(qv, kvbuf[ch, 0]) for ch in chunks]
            return pieces[0] if len(pieces) == 1 else jnp.concatenate(pieces, axis=1)

        s = scores(its[0])
        for i, it in enumerate(its):
            s_n = scores(its[i + 1]) if i + 1 < len(its) else None
            g, half, rs = it
            m_old = mbuf[g, half, rs, :]
            m_new = jnp.maximum(m_old, jnp.max(s, axis=1, keepdims=True))
            alpha = jnp.exp2((m_old - m_new) * EXP2_SCALE)
            p = jnp.exp2((s - m_new[:, :1]) * EXP2_SCALE)
            lbuf[g, half, rs, :] = lbuf[g, half, rs, :] * alpha + lane_sum(p)
            pb = p.astype(BF16)
            o = acc[g, half, rs, :] * alpha
            for i_ch, ch in enumerate(chunks):
                o = o + jnp.dot(pb[:, i_ch * rows:(i_ch + 1) * rows], kvbuf[ch, 1], preferred_element_type=F32)
            acc[g, half, rs, :] = o
            mbuf[g, half, rs, :] = m_new
            s = s_n

    def block_rows(b):
        return pl.ds(pl.multiple_of(b * sub, sub), sub)

    def attend_pair(ch_a, ch_b, pair):
        attend((ch_a, ch_b), [(g, half, block_rows(2 * pair + j)) for half in range(2) for j in range(2) for g in range(2)])

    def attend_last(ch_a, ch_b, b):
        attend((ch_a, ch_b), [(g, half, block_rows(b)) for half in range(2) for g in range(2)])

    def y_copy(src, dst, b, i, dev):
        return remote(src, dst, ys_sem.at[b, i], yr_sem.at[b, i], dev)

    def o_direct(b, i, core):
        return remote(obuf.at[b, first[i], core], orecv.at[b, y, c], ys_sem.at[b, 2 * i + core], yr_sem.at[b, 2 * i + c],
                      {'tp': first[i], 'cp': 2 * x + core})

    def o_direct_wait(b, i, core):
        y_copy(obuf.at[b, y, c], orecv.at[b, first[i], core], b, 2 * i + core, {'tp': y1}).wait_recv()

    def o_far(b, hf, core):
        return remote(obuf.at[b, far, core, hf], orelay.at[b, hf, c], ys_sem.at[b, 4 + 2 * hf + core], yr_sem.at[b, 4 + 2 * hf + c],
                      {'tp': first[hf], 'cp': 2 * x + core})

    def o_far_wait(b, hf, core):
        y_copy(obuf.at[b, far, core, hf], orelay.at[b, hf, core], b, 4 + 2 * hf + core, {'tp': y1}).wait_recv()

    def o_relay(b, hf):
        return y_copy(orelay.at[b, hf], orecv.at[b, first[hf], :, hf], b, 8 + hf, {'tp': second[hf]})

    def o_relay_wait(b, hf):
        y_copy(orelay.at[b, hf], orecv.at[b, far, :, hf], b, 8 + hf, {'tp': y1}).wait_recv()

    def o_partner(b):
        return y_copy(obuf.at[b, y, 1 - c], orecv.at[b, y, c], b, 10, {'cp': partner})

    def o_partner_wait(b):
        y_copy(obuf.at[b, y, c], orecv.at[b, y, 1 - c], b, 10, {'cp': partner}).wait_recv()

    def xt(b, t, hf):
        return out.at[pl.ds(pl.multiple_of(b * sub + t * quarter, quarter), quarter), pl.ds(cols[hf], 512)]

    def ag1_copy(b, hf):
        return y_copy(xt(b, y, hf), xt(b, y, hf), b, 11 + hf, {'tp': second[hf]})

    def ag1_wait(b, hf):
        t = second[hf]
        y_copy(xt(b, t, hf), xt(b, t, hf), b, 11 + hf, {'tp': t}).wait_recv()

    def ag2_copy(b, hf, slot):
        t = y if slot == 0 else second[hf]
        return y_copy(xt(b, t, hf), xt(b, t, hf), b, 13 + 2 * hf + slot, {'tp': first[hf]})

    def ag2_wait(b, hf, slot):
        dev = first[hf]
        t = dev if slot == 0 else far
        y_copy(xt(b, t, hf), xt(b, t, hf), b, 13 + 2 * hf + slot, {'tp': dev}).wait_recv()

    def finish(b):
        rs = block_rows(b)
        for half in range(2):
            for g in range(2):
                den = jnp.sum(lbuf[g, half, rs, :], axis=1, keepdims=True)
                o = (acc[g, half, rs, :] / den).astype(BF16)
                for j in range(4):
                    obuf[b, j, half, g] = o[j * quarter:(j + 1) * quarter, :]
        for hf in range(2):
            for core in range(2):
                o_far(b, hf, core).start()
        for i in range(2):
            for core in range(2):
                o_direct(b, i, core).start()
        o_partner(b).start()
        orecv[b, y, c] = obuf[b, y, c]

    def step1(b):
        for hf in range(2):
            for core in range(2):
                o_far_wait(b, hf, core)
            o_relay(b, hf).start()

    def step2(b):
        own_rows = pl.ds(pl.multiple_of(b * sub + y * quarter, quarter), quarter)

        @pl.when(b == 0)
        def _():
            for i in range(3):
                ref = wo.at[(y1, y2, far)[i], pl.ds(pl.multiple_of((1 - c) * w_half, w_half), w_half)]
                e_copy(ref, ref, 4 + i, {'cp': partner}).wait_recv()
            for hf in range(2):
                mlp_rs1(hf, 0).wait_recv()
                mlp_rs2(hf).wait_recv()

        for i in range(2):
            for core in range(2):
                o_direct_wait(b, i, core)
            o_relay_wait(b, i)
        o_partner_wait(b)
        lhs = jnp.concatenate([orecv[b, src, core, g] for src in range(4) for core in range(2) for g in range(2)], axis=1)
        attn = jnp.dot(lhs, jnp.concatenate([wo[src] for src in range(4)], axis=0), preferred_element_type=F32)
        for hf in range(2):
            at = slice(cols[hf], cols[hf] + 512)
            mlp_tot = mpart[y, hf, b].astype(F32) + mrs1[hf, 0, b].astype(F32) + mrs2[hf, b].astype(F32)
            out[own_rows, at] = (hid[own_rows, at].astype(F32) + attn[:, at] + mlp_tot).astype(BF16)
            ag1_copy(b, hf).start()
        for hf in range(2):
            ag2_copy(b, hf, 0).start()

    def early_sends():
        for cpy in caches:
            cpy.wait()
        dd_kv(own_ch).wait_send()
        dd_q(c).wait_send()

        @pl.when(x < 3)
        def _():
            kv_copy(own_ch, 0, right).wait_send()
            kv_copy(own_ch, 1, right).wait_send()
            kv_copy(oth_ch, 2, right).wait_send()

        @pl.when(x == 0)
        def _():
            kv_copy(oth_ch, 3, left).wait_send()
            kv_copy(oth_ch, 4, left).wait_send()

        @pl.when(x == 1)
        def _():
            kv_copy(own_ch, 3, left).wait_send()

        @pl.when(x == 3)
        def _():
            kv_copy(own_ch, 0, left).wait_send()

        for i in range(2):
            wo_direct(i, y).wait_send()
            wo_relay(i, y1).wait_send()
            mlp_rs2(i).wait_send()
            for slot in range(2):
                mlp_rs1(i, slot).wait_send()
        for i in range(3):
            wo_partner(i).wait_send()

    def step3(b):
        o_partner(b).wait_send()
        for hf in range(2):
            o_relay(b, hf).wait_send()
            for slot in range(2):
                o_direct(b, hf, slot).wait_send()
                o_far(b, hf, slot).wait_send()

        @pl.when(b == blocks - 1)
        def _():
            early_sends()

        for hf in range(2):
            ag1_wait(b, hf)
            ag2_copy(b, hf, 1).start()

    def out_copy(b):
        return pltpu.make_async_copy(out.at[block_rows(b)], out_hbm.at[block_rows(b)], out_sem.at[b])

    def step4(b):
        for hf in range(2):
            ag1_copy(b, hf).wait_send()

            @pl.when(b > 0)
            def _():
                for slot in range(2):
                    ag2_copy(b - 1, hf, slot).wait_send()

        for hf in range(2):
            for slot in range(2):
                ag2_wait(b, hf, slot)
        out_copy(b).start()

    n = 2 * x

    def chunk_of(s):
        first_half = s // 2
        par = s % 2
        near = 2 * (x - 1 - first_half) + (c + par - 2 * c * par)
        mix_half = c + first_half - 2 * c * first_half
        mixed = 4 - 4 * par + mix_half
        late = 2 + (c + par - 2 * c * par)
        three = jnp.where(s < 4, mixed, late)
        return jnp.where(x == 3, three, near)

    three = x == 3
    lead = 2 * (x // 2) + x // 3
    ticks = lead + 8 + 2 * (x // 3)

    def pick(tau, near, far):
        b = jnp.int32(-1)
        for i in range(4):
            b = jnp.where(tau == jnp.where(three, far[i], near[i]), i, b)
        return jnp.maximum(b, 0), b >= 0

    def loop(t, carry):
        tau = t - lead
        gap = jnp.logical_and(three, jnp.logical_or(tau == 0, tau == 3))
        s = jnp.where(t == 2, 2, 0)
        pair = jnp.where(t == 1, 1, 0)

        @pl.when(jnp.logical_and(tau < 0, t != 1))
        def _():
            ch_b = chunk_of(s + 1)
            kv_copy(ch_b, 0, right).wait_recv()

            @pl.when(jnp.logical_and(three, t == 0))
            def _():
                kv_copy(ch_b, 0, left).start()

            @pl.when(x == 2)
            def _():
                kv_copy(ch_b, 1, right).start()

            kv_copy(chunk_of(s), 0, right).wait_recv()

        @pl.when(jnp.logical_and(x > 0, tau == x // 3))
        def _():
            kv_copy(chunk_of(n - 2), 0, right).wait_recv()
            kv_copy(chunk_of(n - 1), 0, right).wait_recv()

            @pl.when(x == 1)
            def _():
                kv_copy(chunk_of(1), 3, right).start()

        @pl.when(t == (x // 2) * (x - 1))
        def _():
            with jax.named_scope('e2'):
                for hf in range(2):
                    mlp_rs1(hf, 1).wait_recv()
                    msum[hf] = (mpart[second[hf], hf].astype(F32) + mrs1[hf, 1].astype(F32)).astype(BF16)
                    mlp_rs2(hf).start()

        @pl.when(tau == x // 3)
        def _():
            with jax.named_scope('e3'):
                for hf in range(2):
                    wo_relay(hf, far).wait_recv()
                for i in range(3):
                    wo_partner(i).start()

        @pl.when(tau < 0)
        def _():
            with jax.named_scope('att'):
                attend_pair(chunk_of(s), chunk_of(s + 1), pair)

        b0, ok0 = pick(tau, (0, 1, 2, 3), (1, 2, 4, 5))

        @pl.when(jnp.logical_and(jnp.logical_or(ok0, gap), x > 0))
        def _():
            back = jnp.where(gap, 4, 2)
            with jax.named_scope('last'):
                attend_last(chunk_of(n - back), chunk_of(n - back + 1), jnp.where(gap, 2 + tau // 3, b0))

        def service(fn, nm, near_t, far_t):
            bk, okk = pick(tau, near_t, far_t)

            @pl.when(okk)
            def _():
                with jax.named_scope(nm):
                    fn(bk)

        service(step3, 's3', (4, 5, 6, 7), (5, 6, 8, 9))
        service(step1, 's1', (1, 2, 3, 4), (2, 3, 5, 6))

        @pl.when(ok0)
        def _():
            with jax.named_scope('finish'):
                finish(b0)

        service(step2, 's2', (2, 3, 4, 5), (3, 4, 6, 7))
        return carry

    lax.fori_loop(0, ticks, loop, 0)

    def last_step(b, carry):
        with jax.named_scope('s4'):
            step4(b)
        return carry

    lax.fori_loop(0, blocks, last_step, 0)

    for hf in range(2):
        for slot in range(2):
            ag2_copy(blocks - 1, hf, slot).wait_send()
    for b in range(blocks):
        out_copy(b).wait()


def layer(hidden, positions, gain, w_q, w_k, w_v, w_gate, w_up, w_down, w_o):
    rows, width = hidden.shape
    ff = w_gate.shape[1]
    hr = 256
    nb = rows // hr
    qr = hr // 4
    hw = width // 2
    freq = 1.0 / (ROPE_BASE ** (np.repeat(np.arange(0, HEAD_DIM, 2), 2) / HEAD_DIM))
    freq = jnp.asarray(freq[None, :], F32)
    anyspec = pl.BlockSpec(memory_space=pl.ANY)
    vm = pltpu.VMEM
    dma = pltpu.SemaphoreType.DMA
    return pl.pallas_call(
        layer_kernel,
        in_specs=[anyspec] * 11,
        out_specs=[anyspec] * 3,
        out_shape=[jax.ShapeDtypeStruct((rows, width), BF16),
                   jax.ShapeDtypeStruct((rows * w_k.shape[1] // HEAD_DIM, HEAD_DIM), BF16),
                   jax.ShapeDtypeStruct((rows * w_v.shape[1] // HEAD_DIM, HEAD_DIM), BF16)],
        scratch_shapes=[
            vm((8, 2, rows, HEAD_DIM), BF16),
            vm((2, 2, rows, HEAD_DIM), BF16),
            vm((2, rows, HEAD_DIM), BF16),
            vm((2, rows, HEAD_DIM), BF16),
            vm((2, 2, rows, HEAD_DIM), F32),
            vm((2, 2, rows, HEAD_DIM), F32),
            vm((2, 2, rows, HEAD_DIM), F32),
            vm((rows, width), BF16),
            vm((rows, width), BF16),
            vm((rows // HEAD_DIM, HEAD_DIM), jnp.int32),
            vm((width // HEAD_DIM, HEAD_DIM), BF16),
            vm((1, HEAD_DIM), F32),
            vm((rows, HEAD_DIM), F32),
            vm((rows, HEAD_DIM), F32),
            vm(w_q.shape, BF16), vm(w_k.shape, BF16), vm(w_v.shape, BF16),
            vm((width, ff), BF16), vm((width, ff), BF16), vm((ff, width), BF16),
            vm((4,) + w_o.shape, BF16),
            vm((2, 2 * hr, HEAD_DIM), F32),
            vm((rows * w_k.shape[1] // HEAD_DIM, HEAD_DIM), BF16),
            vm((rows * w_v.shape[1] // HEAD_DIM, HEAD_DIM), BF16),
            vm((4, 2, nb, qr, hw), BF16),
            vm((2, 2, nb, qr, hw), BF16),
            vm((2, nb, qr, hw), BF16),
            vm((2, nb, qr, hw), BF16),
            vm((nb, 4, 2, 2, qr, HEAD_DIM), BF16),
            vm((nb, 4, 2, 2, qr, HEAD_DIM), BF16),
            vm((nb, 2, 2, qr, HEAD_DIM), BF16),
            vm((rows, width), BF16),
            dma((13,)), dma((nb,)), dma((5, 2)), dma((8, 2)), dma((2,)), dma((2,)), dma((13,)), dma((13,)),
            dma((nb, 17)), dma((nb, 17)), dma((nb,)),
        ],
        compiler_params=pltpu.CompilerParams(collective_id=0, has_side_effects=True, vmem_limit_bytes=62 << 20),
        name='layer',
    )(hidden, positions.reshape(rows // HEAD_DIM, HEAD_DIM), gain.reshape(width // HEAD_DIM, HEAD_DIM), freq,
      w_q, w_k, w_v, w_gate, w_up, w_down, w_o)


def solution(mesh):
    def local_layer(hidden, positions, ln_gain, w_q, w_k, w_v, w_o, w_gate, w_up, w_down):
        rows = hidden.shape[0]
        kv_local = w_k.shape[1] // HEAD_DIM
        out, kc, vc = layer(hidden, positions, ln_gain, w_q, w_k, w_v, w_gate, w_up, w_down, w_o)
        return out, kc.reshape(rows, kv_local, HEAD_DIM), vc.reshape(rows, kv_local, HEAD_DIM)

    row_spec = P(('dp', 'cp'), None)
    col_spec = P(None, 'tp')
    cache_spec = P(('dp', 'cp'), 'tp', None)
    in_specs = (row_spec, P(('dp', 'cp')), P(None), col_spec, col_spec, col_spec, P('tp', None), col_spec, col_spec, P('tp', None))
    return jax.shard_map(local_layer, mesh=mesh, in_specs=in_specs, out_specs=(row_spec, cache_spec, cache_spec), check_vma=False)
```

```python
import jax
import jax.numpy as jnp
import numpy as np
from jax import lax
from jax.experimental import pallas as pl
from jax.experimental.pallas import tpu as pltpu
from jax.sharding import PartitionSpec as P

HEAD_DIM = 128
ROPE_BASE = 4000000
LN_EPS = 1e-5
EXP2_SCALE = (HEAD_DIM ** -0.5) * 1.4426950408889634
MESH = pl.DeviceIdType.MESH
BF16 = jnp.bfloat16
F32 = jnp.float32


def sin_cos(angle):
    k = jnp.floor(angle * 0.6366197723675814 + 0.5)
    r = ((angle - k * 1.5703125) - k * 4.837512969970703125e-4) - k * 7.54978995489188216e-8
    z = r * r
    sn = r + r * z * (-1.6666654611e-1 + z * (8.3321608736e-3 - 1.9515295891e-4 * z))
    cs = 1.0 - 0.5 * z + z * z * (4.166664568298827e-2 + z * (-1.388731625493765e-3 + z * 2.443315711809948e-5))
    quad = k.astype(jnp.int32)
    odd = (quad & 1) == 1
    sin = jnp.where(odd, cs, sn)
    cos = jnp.where(odd, sn, cs)
    sin = jnp.where((quad & 2) == 2, -sin, sin)
    cos = jnp.where(((quad + 1) & 2) == 2, -cos, cos)
    return sin, cos


def layer_kernel(hid_hbm, pos_hbm, gain_hbm, freq_hbm, wq_hbm, wk_hbm, wv_hbm, wg_hbm, wu_hbm, wd_hbm, wo_hbm,
                 out_hbm, kc_hbm, vc_hbm,
                 kvbuf, qbuf, acc, mbuf, lbuf, hid, h, pos, gain, freq, cost, sint,
                 wq, wk, wv, wg, wu, wd, wo, wide, kc, vc,
                 mpart, mrs1, msum, mrs2, obuf, orecv, orelay, out,
                 load_sem, hid_sem, kvs_sem, kvr_sem, dds_sem, ddr_sem, es_sem, er_sem, ys_sem, yr_sem, out_sem):
    cp = lax.axis_index('cp')
    y = lax.axis_index('tp')
    x = cp // 2
    c = cp % 2
    partner = 2 * x + 1 - c
    right = ((x + 1) % 4) * 2 + c
    left = ((x + 3) % 4) * 2 + c
    y1 = y + 1 - 2 * (y % 2)
    y2 = 3 - y
    rows = hid_hbm.shape[0]
    sub = 256
    blocks = rows // sub
    straight = 2
    quarter = sub // 4

    barrier = pltpu.get_barrier_semaphore()
    for dev in ({'cp': partner}, {'cp': right}, {'cp': left}, {'tp': y1}, {'tp': y2},
                {'tp': y1, 'cp': partner}, {'tp': y2, 'cp': partner}, {'tp': 3 - y1}, {'tp': 3 - y1, 'cp': partner}):
        pl.semaphore_signal(barrier, inc=1, device_id=dev, device_id_type=MESH)

    pairs = ((hid_hbm, hid), (pos_hbm, pos), (gain_hbm, gain), (freq_hbm, freq), (wk_hbm, wk), (wv_hbm, wv), (wq_hbm, wq),
             (wg_hbm, wg), (wu_hbm, wu), (wd_hbm, wd), (wo_hbm, wo.at[y]))
    loads = [pltpu.make_async_copy(src, dst, load_sem.at[i]) for i, (src, dst) in enumerate(pairs)]
    def hid_tile(i):
        rs = pl.ds(pl.multiple_of(i * sub, sub), sub)
        return pltpu.make_async_copy(hid_hbm.at[rs], hid.at[rs], hid_sem.at[i])

    loads[1].start()
    loads[3].start()
    hid_tile(0).start()
    for i in (2, 4, 5):
        loads[i].start()
    for i in range(1, blocks):
        hid_tile(i).start()
    for i in (6, 10):
        loads[i].start()

    def remote(src, dst, ss, rsem, dev):
        return pltpu.make_async_remote_copy(src_ref=src, dst_ref=dst, send_sem=ss, recv_sem=rsem,
                                            device_id=dev, device_id_type=MESH)

    def dd_kv(ch):
        return remote(kvbuf.at[spare], kvbuf.at[ch], dds_sem.at[0], ddr_sem.at[0], {'cp': partner})

    def dd_q(half):
        return remote(qbuf.at[2], qbuf.at[half], dds_sem.at[1], ddr_sem.at[1], {'cp': partner})

    class KvCopy:
        def __init__(self, ch, slot, dev):
            self.parts = []
            for p in range(2):
                ref = kvbuf.at[ch, :, pl.ds(p * (rows // 2), rows // 2)]
                self.parts.append(remote(ref, ref, kvs_sem.at[slot, p], kvr_sem.at[ch, p], {'cp': dev}))

        def start(self):
            for part in self.parts:
                part.start()

        def wait_recv(self):
            for part in self.parts:
                part.wait_recv()

        def wait_send(self):
            for part in self.parts:
                part.wait_send()

    kv_copy = KvCopy

    first = (y1, y2)
    second = (y2, y1)
    far = 3 - y1

    def e_copy(src, dst, i, dev):
        return remote(src, dst, es_sem.at[i], er_sem.at[i], dev)

    w_half = 2 * HEAD_DIM

    def wo_rows(shard, lo, size):
        return wo.at[shard, pl.ds(pl.multiple_of(c * w_half + lo, HEAD_DIM), size)]

    def wo_direct(i, shard):
        ref = wo_rows(shard, 0, w_half)
        return e_copy(ref, ref, i, {'tp': first[i]})

    def wo_relay(hf, shard):
        ref = wo_rows(shard, hf * HEAD_DIM, HEAD_DIM)
        return e_copy(ref, ref, 2 + hf, {'tp': first[hf]})

    def wo_partner(i):
        ref = wo_rows((y1, y2, far)[i], 0, w_half)
        return e_copy(ref, ref, 4 + i, {'cp': partner})

    def mlp_rs1(hf, slot):
        dev = first[hf]
        beyond = (3 - dev) if hf == 0 else (dev + 1 - 2 * (dev % 2))
        tile = dev if slot == 0 else beyond
        return e_copy(mpart.at[tile, hf], mrs1.at[hf, slot], 7 + 2 * hf + slot, {'tp': dev})

    def mlp_rs2(hf):
        return e_copy(msum.at[hf], mrs2.at[hf], 11 + hf, {'tp': second[hf]})

    own_ch = 2 * x + c
    spare = kvbuf.shape[0] - 1
    oth_ch = 2 * x + 1 - c

    loads[1].wait()
    loads[3].wait()
    lane = lax.broadcasted_iota(jnp.int32, (HEAD_DIM, HEAD_DIM), 1)
    for i in range(rows // HEAD_DIM):
        at = pl.ds(i * HEAD_DIM, HEAD_DIM)
        p = jnp.broadcast_to(pos[i:i + 1, :].astype(F32), (HEAD_DIM, HEAD_DIM)).T
        sn, cs = sin_cos(p * freq[...])
        cost[at, :] = cs
        sint[at, :] = jnp.where(lane % 2 == 0, -sn, sn)
    for i in (7, 8, 9):
        loads[i].start()
    for i in (2, 4, 5):
        loads[i].wait()

    even = lax.broadcasted_iota(jnp.int32, (sub, HEAD_DIM), 1) % 2 == 0
    gain_f = gain[...].astype(F32)
    gain_row = jnp.concatenate([gain_f[i:i + 1, :] for i in range(gain.shape[0])], axis=1)

    def rope(col, rs):
        u = col.astype(BF16).astype(F32)
        swapped = jnp.where(even, pltpu.roll(u, HEAD_DIM - 1, 1), pltpu.roll(u, 1, 1))
        return (u * cost[rs, :] + swapped * sint[rs, :]).astype(BF16)

    def project_kv(i, carry):
        rs = pl.ds(pl.multiple_of(i * sub, sub), sub)
        hid_tile(i).wait()
        xx = hid[rs, :].astype(F32)
        cent = xx - jnp.mean(xx, axis=-1, keepdims=True)
        var = jnp.mean(cent * cent, axis=-1, keepdims=True)
        hh = (cent * lax.rsqrt(var + LN_EPS) * gain_row).astype(BF16)
        h[rs, :] = hh
        k = jnp.dot(hh, wk[...], preferred_element_type=F32)
        v = jnp.dot(hh, wv[...], preferred_element_type=F32).astype(BF16)
        kk = [rope(k[:, g * HEAD_DIM:(g + 1) * HEAD_DIM], rs) for g in range(2)]
        vv = [v[:, g * HEAD_DIM:(g + 1) * HEAD_DIM] for g in range(2)]
        pair_rows = pl.ds(pl.multiple_of(i * 2 * sub, 2 * sub), 2 * sub)
        for slot, (vals, out) in enumerate(((kk, kc), (vv, vc))):
            for g in range(2):
                wide[slot, pl.ds(g, sub, 2), :] = vals[g].astype(F32)
            out[pair_rows, :] = wide[slot].astype(BF16)

        for g in range(2):
            to = jnp.where(c == g, own_ch, spare)
            kvbuf[to, 0, rs, :] = kk[g]
            kvbuf[to, 1, rs, :] = vv[g]
        return carry

    def send_own(p):
        @pl.when(x < 3)
        def _():
            kv_copy(own_ch, 0, right).parts[p].start()

        @pl.when(x < 2)
        def _():
            kv_copy(own_ch, 1, left).parts[p].start()

    with jax.named_scope('kvproj'):
        lax.fori_loop(0, blocks // 2, project_kv, 0)
    with jax.named_scope('bar'):
        pl.semaphore_wait(barrier, 9)
    send_own(0)
    with jax.named_scope('kvproj'):
        lax.fori_loop(blocks // 2, blocks, project_kv, 0)
    send_own(1)
    dd_kv(own_ch).start()

    loads[10].wait()
    for i in range(2):
        wo_direct(i, y).start()

    caches = (pltpu.make_async_copy(kc, kc_hbm, load_sem.at[11]), pltpu.make_async_copy(vc, vc_hbm, load_sem.at[12]))
    for cpy in caches:
        cpy.start()
    loads[6].wait()

    def project_q(i, carry):
        rs = pl.ds(pl.multiple_of(i * sub, sub), sub)
        q = jnp.dot(h[rs, :], wq[...], preferred_element_type=F32)
        for g in range(2):
            for j in range(2):
                lo = (2 * g + j) * HEAD_DIM
                qr = rope(q[:, lo:lo + HEAD_DIM], rs)

                qbuf[jnp.where(c == g, c, 2), j, rs, :] = qr
        return carry

    with jax.named_scope('qproj'):
        lax.fori_loop(0, rows // sub, project_q, 0)
    dd_q(c).start()
    dd_kv(oth_ch).wait_recv()

    @pl.when(x < 3)
    def _():
        kv_copy(oth_ch, 2, right).start()

    @pl.when(x == 0)
    def _():
        kv_copy(oth_ch, 3, left).start()

    loads[7].wait()
    loads[8].wait()
    loads[9].wait()

    cols = (0, 512)

    def mlp(i, carry):
        rs = pl.ds(pl.multiple_of(i * sub, sub), sub)
        hh = h[rs, :]
        gate = jnp.dot(hh, wg[...], preferred_element_type=F32).astype(BF16).astype(F32)
        up = jnp.dot(hh, wu[...], preferred_element_type=F32).astype(BF16).astype(F32)
        a = (gate * (1.0 / (1.0 + jnp.exp(-gate))) * up).astype(BF16)
        tot = jnp.dot(a, wd[...], preferred_element_type=F32).astype(BF16)
        for j in range(4):
            for hf in range(2):
                mpart[j, hf, i] = tot[j * quarter:(j + 1) * quarter, cols[hf]:cols[hf] + 512]
        return carry

    with jax.named_scope('mlp'):
        lax.fori_loop(0, rows // sub, mlp, 0)

    for slot in (1, 0):
        for hf in range(2):
            mlp_rs1(hf, slot).start()
    dd_q(1 - c).wait_recv()

    def lane_sum(p):
        s = p[:, :HEAD_DIM]
        for j in range(1, p.shape[1] // HEAD_DIM):
            s = s + p[:, j * HEAD_DIM:(j + 1) * HEAD_DIM]
        return s

    def qk(qv, kv):
        return lax.dot_general(qv, kv, (((1,), (1,)), ((), ())), preferred_element_type=F32)

    k0, k1, v0, v1 = (kvbuf.at[2 * x, 0], kvbuf.at[2 * x + 1, 0], kvbuf.at[2 * x, 1], kvbuf.at[2 * x + 1, 1])
    tri = (lax.broadcasted_iota(jnp.int32, (sub, sub), 1) <= lax.broadcasted_iota(jnp.int32, (sub, sub), 0))
    groups = rows // sub

    def diag_scores(r, g):
        half, off = r // groups, (r % groups) * sub
        qv = qbuf[half, g, pl.ds(off, sub), :]
        pieces = []
        if half == 1:
            pieces.append(qk(qv, k0[...]))
        kk = k0 if half == 0 else k1
        if off:
            pieces.append(qk(qv, kk[pl.ds(0, off), :]))
        pieces.append(jnp.where(tri, qk(qv, kk[pl.ds(off, sub), :]), -jnp.inf))
        return pieces[0] if len(pieces) == 1 else jnp.concatenate(pieces, axis=1)

    def diag_soft(r, g, s):
        half, off = r // groups, (r % groups) * sub
        rs = pl.ds(off, sub)
        mx = jnp.max(s, axis=1, keepdims=True)
        p = jnp.exp2((s - mx) * EXP2_SCALE)
        pb = p.astype(BF16)
        if half == 0:
            o = jnp.dot(pb, v0[pl.ds(0, off + sub), :], preferred_element_type=F32)
        else:
            o = jnp.dot(pb[:, :rows], v0[...], preferred_element_type=F32)
            o = o + jnp.dot(pb[:, rows:], v1[pl.ds(0, off + sub), :], preferred_element_type=F32)
        mbuf[g, half, rs, :] = jnp.broadcast_to(mx, (sub, HEAD_DIM))
        lbuf[g, half, rs, :] = lane_sum(p)
        acc[g, half, rs, :] = o

    items = [(r, g) for r in range(2 * groups) for g in range(2)]
    own_block = jax.named_scope('diag')
    own_block.__enter__()
    s_now = diag_scores(*items[0])
    for i, it in enumerate(items):
        s_next = diag_scores(*items[i + 1]) if i + 1 < len(items) else None
        diag_soft(*it, s_now)
        s_now = s_next

    own_block.__exit__(None, None, None)
    for hf in range(2):
        wo_direct(1 - hf, second[hf]).wait_recv()
        wo_relay(hf, second[hf]).start()

    @pl.when(x == 0)
    def _():
        kv_copy(2 + c, 0, right).wait_recv()
        kv_copy(2 + c, 4, left).start()

    def attend(chunks, its):
        def scores(it):
            g, half, rs = it
            qv = qbuf[half, g, rs, :]
            pieces = [qk(qv, kvbuf[ch, 0]) for ch in chunks]
            return pieces[0] if len(pieces) == 1 else jnp.concatenate(pieces, axis=1)

        s = scores(its[0])
        for i, it in enumerate(its):
            s_n = scores(its[i + 1]) if i + 1 < len(its) else None
            g, half, rs = it
            m_old = mbuf[g, half, rs, :]
            m_new = jnp.maximum(m_old, jnp.max(s, axis=1, keepdims=True))
            alpha = jnp.exp2((m_old - m_new) * EXP2_SCALE)
            p = jnp.exp2((s - m_new[:, :1]) * EXP2_SCALE)
            lbuf[g, half, rs, :] = lbuf[g, half, rs, :] * alpha + lane_sum(p)
            pb = p.astype(BF16)
            o = acc[g, half, rs, :] * alpha
            for i_ch, ch in enumerate(chunks):
                o = o + jnp.dot(pb[:, i_ch * rows:(i_ch + 1) * rows], kvbuf[ch, 1], preferred_element_type=F32)
            acc[g, half, rs, :] = o
            mbuf[g, half, rs, :] = m_new
            s = s_n

    def block_rows(b):
        return pl.ds(pl.multiple_of(b * sub, sub), sub)

    def attend_pair(ch_a, ch_b, pair):
        attend((ch_a, ch_b), [(g, half, block_rows(2 * pair + j)) for half in range(2) for j in range(2) for g in range(2)])

    def attend_last(ch_a, ch_b, b):
        attend((ch_a, ch_b), [(g, half, block_rows(b)) for half in range(2) for g in range(2)])

    def y_copy(src, dst, b, i, dev):
        return remote(src, dst, ys_sem.at[b, i], yr_sem.at[b, i], dev)

    def o_direct(b, i, core):
        return remote(obuf.at[b, first[i], core], orecv.at[b, y, c], ys_sem.at[b, 2 * i + core], yr_sem.at[b, 2 * i + c],
                      {'tp': first[i], 'cp': 2 * x + core})

    def o_direct_wait(b, i, core):
        y_copy(obuf.at[b, y, c], orecv.at[b, first[i], core], b, 2 * i + core, {'tp': y1}).wait_recv()

    def o_far(b, hf, core):
        return remote(obuf.at[b, far, core, hf], orelay.at[b, hf, c], ys_sem.at[b, 4 + 2 * hf + core], yr_sem.at[b, 4 + 2 * hf + c],
                      {'tp': first[hf], 'cp': 2 * x + core})

    def o_far_wait(b, hf, core):
        y_copy(obuf.at[b, far, core, hf], orelay.at[b, hf, core], b, 4 + 2 * hf + core, {'tp': y1}).wait_recv()

    def o_relay(b, hf):
        return y_copy(orelay.at[b, hf], orecv.at[b, first[hf], :, hf], b, 8 + hf, {'tp': second[hf]})

    def o_relay_wait(b, hf):
        y_copy(orelay.at[b, hf], orecv.at[b, far, :, hf], b, 8 + hf, {'tp': y1}).wait_recv()

    def o_beyond(b, core):
        return remote(obuf.at[b, far, core], orecv.at[b, y, c], ys_sem.at[b, 4 + core], yr_sem.at[b, 4 + c],
                      {'tp': far, 'cp': 2 * x + core})

    def o_beyond_wait(b, core):
        y_copy(obuf.at[b, y, c], orecv.at[b, far, core], b, 4 + core, {'tp': far}).wait_recv()

    def o_partner(b):
        return y_copy(obuf.at[b, y, 1 - c], orecv.at[b, y, c], b, 10, {'cp': partner})

    def o_partner_wait(b):
        y_copy(obuf.at[b, y, c], orecv.at[b, y, 1 - c], b, 10, {'cp': partner}).wait_recv()

    def xt(b, t, hf):
        return out.at[pl.ds(pl.multiple_of(b * sub + t * quarter, quarter), quarter), pl.ds(cols[hf], 512)]

    def ag1_copy(b, hf):
        return y_copy(xt(b, y, hf), xt(b, y, hf), b, 11 + hf, {'tp': second[hf]})

    def ag1_wait(b, hf):
        t = second[hf]
        y_copy(xt(b, t, hf), xt(b, t, hf), b, 11 + hf, {'tp': t}).wait_recv()

    def ag2_copy(b, hf, slot):
        t = y if slot == 0 else second[hf]
        return y_copy(xt(b, t, hf), xt(b, t, hf), b, 13 + 2 * hf + slot, {'tp': first[hf]})

    def ag2_wait(b, hf, slot):
        dev = first[hf]
        t = dev if slot == 0 else far
        y_copy(xt(b, t, hf), xt(b, t, hf), b, 13 + 2 * hf + slot, {'tp': dev}).wait_recv()

    def finish(b):
        rs = block_rows(b)
        for half in range(2):
            for g in range(2):
                den = jnp.sum(lbuf[g, half, rs, :], axis=1, keepdims=True)
                o = (acc[g, half, rs, :] / den).astype(BF16)
                for j in range(4):
                    obuf[b, j, half, g] = o[j * quarter:(j + 1) * quarter, :]
        @pl.when(b < straight)
        def _():
            for hf in range(2):
                for core in range(2):
                    o_far(b, hf, core).start()

        @pl.when(b >= straight)
        def _():
            for core in range(2):
                o_beyond(b, core).start()

        for i in range(2):
            for core in range(2):
                o_direct(b, i, core).start()
        o_partner(b).start()
        orecv[b, y, c] = obuf[b, y, c]

    def step1(b):
        @pl.when(b < straight)
        def _():
            for hf in range(2):
                for core in range(2):
                    o_far_wait(b, hf, core)
                o_relay(b, hf).start()

    def step2(b):
        own_rows = pl.ds(pl.multiple_of(b * sub + y * quarter, quarter), quarter)

        @pl.when(b == 0)
        def _():
            for i in range(3):
                ref = wo.at[(y1, y2, far)[i], pl.ds(pl.multiple_of((1 - c) * w_half, w_half), w_half)]
                e_copy(ref, ref, 4 + i, {'cp': partner}).wait_recv()
            for hf in range(2):
                mlp_rs1(hf, 0).wait_recv()
                mlp_rs2(hf).wait_recv()

        for i in range(2):
            for core in range(2):
                o_direct_wait(b, i, core)

        @pl.when(b < straight)
        def _():
            for hf in range(2):
                o_relay_wait(b, hf)

        @pl.when(b >= straight)
        def _():
            for core in range(2):
                o_beyond_wait(b, core)

        o_partner_wait(b)
        lhs = jnp.concatenate([orecv[b, src, core, g] for src in range(4) for core in range(2) for g in range(2)], axis=1)
        attn = jnp.dot(lhs, jnp.concatenate([wo[src] for src in range(4)], axis=0), preferred_element_type=F32)
        for hf in range(2):
            at = slice(cols[hf], cols[hf] + 512)
            mlp_tot = mpart[y, hf, b].astype(F32) + mrs1[hf, 0, b].astype(F32) + mrs2[hf, b].astype(F32)
            out[own_rows, at] = (hid[own_rows, at].astype(F32) + attn[:, at] + mlp_tot).astype(BF16)
            ag1_copy(b, hf).start()
        for hf in range(2):
            ag2_copy(b, hf, 0).start()

    def early_sends():
        for cpy in caches:
            cpy.wait()
        dd_kv(own_ch).wait_send()
        dd_q(c).wait_send()

        @pl.when(x < 3)
        def _():
            kv_copy(own_ch, 0, right).wait_send()
            kv_copy(own_ch, 1, right).wait_send()
            kv_copy(oth_ch, 2, right).wait_send()

        @pl.when(x == 0)
        def _():
            kv_copy(oth_ch, 3, left).wait_send()
            kv_copy(oth_ch, 4, left).wait_send()

        @pl.when(x == 1)
        def _():
            kv_copy(own_ch, 3, left).wait_send()

        @pl.when(x == 3)
        def _():
            kv_copy(own_ch, 0, left).wait_send()

        for i in range(2):
            wo_direct(i, y).wait_send()
            wo_relay(i, y1).wait_send()
            mlp_rs2(i).wait_send()
            for slot in range(2):
                mlp_rs1(i, slot).wait_send()
        for i in range(3):
            wo_partner(i).wait_send()

    def step3(b):
        o_partner(b).wait_send()
        for i in range(2):
            for core in range(2):
                o_direct(b, i, core).wait_send()

        @pl.when(b < straight)
        def _():
            for hf in range(2):
                o_relay(b, hf).wait_send()
                for core in range(2):
                    o_far(b, hf, core).wait_send()

        @pl.when(b >= straight)
        def _():
            for core in range(2):
                o_beyond(b, core).wait_send()

        @pl.when(b == blocks - 1)
        def _():
            early_sends()

        for hf in range(2):
            ag1_wait(b, hf)
            ag2_copy(b, hf, 1).start()

    def out_copy(b):
        return pltpu.make_async_copy(out.at[block_rows(b)], out_hbm.at[block_rows(b)], out_sem.at[b])

    def step4(b):
        for hf in range(2):
            ag1_copy(b, hf).wait_send()

            @pl.when(b > 0)
            def _():
                for slot in range(2):
                    ag2_copy(b - 1, hf, slot).wait_send()

        for hf in range(2):
            for slot in range(2):
                ag2_wait(b, hf, slot)
        out_copy(b).start()

    n = 2 * x

    def chunk_of(s):
        first_half = s // 2
        par = s % 2
        near = 2 * (x - 1 - first_half) + (c + par - 2 * c * par)
        mix_half = c + first_half - 2 * c * first_half
        mixed = 4 - 4 * par + mix_half
        late = 2 + (c + par - 2 * c * par)
        three = jnp.where(s < 4, mixed, late)
        return jnp.where(x == 3, three, near)

    three = x == 3
    lead = 2 * (x // 2) + x // 3
    ticks = lead + 8 + 2 * (x // 3)

    def pick(tau, near, far):
        b = jnp.int32(-1)
        for i in range(4):
            b = jnp.where(tau == jnp.where(three, far[i], near[i]), i, b)
        return jnp.maximum(b, 0), b >= 0

    def loop(t, carry):
        tau = t - lead
        gap = jnp.logical_and(three, jnp.logical_or(tau == 0, tau == 3))
        s = jnp.where(t == 2, 2, 0)
        pair = jnp.where(t == 1, 1, 0)

        @pl.when(jnp.logical_and(tau < 0, t != 1))
        def _():
            ch_b = chunk_of(s + 1)
            kv_copy(ch_b, 0, right).wait_recv()

            @pl.when(jnp.logical_and(three, t == 0))
            def _():
                kv_copy(ch_b, 0, left).start()

            @pl.when(x == 2)
            def _():
                kv_copy(ch_b, 1, right).start()

            kv_copy(chunk_of(s), 0, right).wait_recv()

        @pl.when(jnp.logical_and(x > 0, tau == x // 3))
        def _():
            kv_copy(chunk_of(n - 2), 0, right).wait_recv()
            kv_copy(chunk_of(n - 1), 0, right).wait_recv()

            @pl.when(x == 1)
            def _():
                kv_copy(chunk_of(1), 3, right).start()

        @pl.when(t == (x // 2) * (x - 1))
        def _():
            with jax.named_scope('e2'):
                for hf in range(2):
                    mlp_rs1(hf, 1).wait_recv()
                    msum[hf] = (mpart[second[hf], hf].astype(F32) + mrs1[hf, 1].astype(F32)).astype(BF16)
                    mlp_rs2(hf).start()

        @pl.when(tau == x // 3)
        def _():
            with jax.named_scope('e3'):
                for hf in range(2):
                    wo_relay(hf, far).wait_recv()
                for i in range(3):
                    wo_partner(i).start()

        @pl.when(tau < 0)
        def _():
            with jax.named_scope('att'):
                attend_pair(chunk_of(s), chunk_of(s + 1), pair)

        b0, ok0 = pick(tau, (0, 1, 2, 3), (1, 2, 4, 5))

        @pl.when(jnp.logical_and(jnp.logical_or(ok0, gap), x > 0))
        def _():
            back = jnp.where(gap, 4, 2)
            with jax.named_scope('last'):
                attend_last(chunk_of(n - back), chunk_of(n - back + 1), jnp.where(gap, 2 + tau // 3, b0))

        def service(fn, nm, near_t, far_t):
            bk, okk = pick(tau, near_t, far_t)

            @pl.when(okk)
            def _():
                with jax.named_scope(nm):
                    fn(bk)

        service(step3, 's3', (4, 5, 6, 7), (5, 6, 8, 9))
        service(step1, 's1', (1, 2, 3, 4), (2, 3, 5, 6))

        @pl.when(ok0)
        def _():
            with jax.named_scope('finish'):
                finish(b0)

        service(step2, 's2', (2, 3, 4, 5), (3, 4, 5, 7))
        return carry

    lax.fori_loop(0, ticks, loop, 0)

    def last_step(b, carry):
        with jax.named_scope('s4'):
            step4(b)
        return carry

    lax.fori_loop(0, blocks, last_step, 0)

    with jax.named_scope('sends'):
        for hf in range(2):
            for slot in range(2):
                ag2_copy(blocks - 1, hf, slot).wait_send()
    with jax.named_scope('outs'):
        for b in range(blocks):
            out_copy(b).wait()


def layer(hidden, positions, gain, w_q, w_k, w_v, w_gate, w_up, w_down, w_o):
    rows, width = hidden.shape
    ff = w_gate.shape[1]
    hr = 256
    nb = rows // hr
    qr = hr // 4
    hw = width // 2
    freq = 1.0 / (ROPE_BASE ** (np.repeat(np.arange(0, HEAD_DIM, 2), 2) / HEAD_DIM))
    freq = jnp.asarray(freq[None, :], F32)
    anyspec = pl.BlockSpec(memory_space=pl.ANY)
    vm = pltpu.VMEM
    dma = pltpu.SemaphoreType.DMA
    return pl.pallas_call(
        layer_kernel,
        in_specs=[anyspec] * 11,
        out_specs=[anyspec] * 3,
        out_shape=[jax.ShapeDtypeStruct((rows, width), BF16),
                   jax.ShapeDtypeStruct((rows * w_k.shape[1] // HEAD_DIM, HEAD_DIM), BF16),
                   jax.ShapeDtypeStruct((rows * w_v.shape[1] // HEAD_DIM, HEAD_DIM), BF16)],
        scratch_shapes=[
            vm((9, 2, rows, HEAD_DIM), BF16),
            vm((3, 2, rows, HEAD_DIM), BF16),
            vm((2, 2, rows, HEAD_DIM), F32),
            vm((2, 2, rows, HEAD_DIM), F32),
            vm((2, 2, rows, HEAD_DIM), F32),
            vm((rows, width), BF16),
            vm((rows, width), BF16),
            vm((rows // HEAD_DIM, HEAD_DIM), jnp.int32),
            vm((width // HEAD_DIM, HEAD_DIM), BF16),
            vm((1, HEAD_DIM), F32),
            vm((rows, HEAD_DIM), F32),
            vm((rows, HEAD_DIM), F32),
            vm(w_q.shape, BF16), vm(w_k.shape, BF16), vm(w_v.shape, BF16),
            vm((width, ff), BF16), vm((width, ff), BF16), vm((ff, width), BF16),
            vm((4,) + w_o.shape, BF16),
            vm((2, 2 * hr, HEAD_DIM), F32),
            vm((rows * w_k.shape[1] // HEAD_DIM, HEAD_DIM), BF16),
            vm((rows * w_v.shape[1] // HEAD_DIM, HEAD_DIM), BF16),
            vm((4, 2, nb, qr, hw), BF16),
            vm((2, 2, nb, qr, hw), BF16),
            vm((2, nb, qr, hw), BF16),
            vm((2, nb, qr, hw), BF16),
            vm((nb, 4, 2, 2, qr, HEAD_DIM), BF16),
            vm((nb, 4, 2, 2, qr, HEAD_DIM), BF16),
            vm((nb, 2, 2, qr, HEAD_DIM), BF16),
            vm((rows, width), BF16),
            dma((13,)), dma((nb,)), dma((5, 2)), dma((8, 2)), dma((2,)), dma((2,)), dma((13,)), dma((13,)),
            dma((nb, 17)), dma((nb, 17)), dma((nb,)),
        ],
        compiler_params=pltpu.CompilerParams(collective_id=0, has_side_effects=True, vmem_limit_bytes=62 << 20),
        name='layer',
    )(hidden, positions.reshape(rows // HEAD_DIM, HEAD_DIM), gain.reshape(width // HEAD_DIM, HEAD_DIM), freq,
      w_q, w_k, w_v, w_gate, w_up, w_down, w_o)


def solution(mesh):
    def local_layer(hidden, positions, ln_gain, w_q, w_k, w_v, w_o, w_gate, w_up, w_down):
        rows = hidden.shape[0]
        kv_local = w_k.shape[1] // HEAD_DIM
        out, kc, vc = layer(hidden, positions, ln_gain, w_q, w_k, w_v, w_gate, w_up, w_down, w_o)
        return out, kc.reshape(rows, kv_local, HEAD_DIM), vc.reshape(rows, kv_local, HEAD_DIM)

    row_spec = P(('dp', 'cp'), None)
    col_spec = P(None, 'tp')
    cache_spec = P(('dp', 'cp'), 'tp', None)
    in_specs = (row_spec, P(('dp', 'cp')), P(None), col_spec, col_spec, col_spec, P('tp', None), col_spec, col_spec, P('tp', None))
    return jax.shard_map(local_layer, mesh=mesh, in_specs=in_specs, out_specs=(row_spec, cache_spec, cache_spec), check_vma=False)
```

```python
import jax
import jax.numpy as jnp
import numpy as np
from jax import lax
from jax.experimental import pallas as pl
from jax.experimental.pallas import tpu as pltpu
from jax.sharding import PartitionSpec as P

HEAD_DIM = 128
ROPE_BASE = 4000000
LN_EPS = 1e-5
EXP2_SCALE = (HEAD_DIM ** -0.5) * 1.4426950408889634
MESH = pl.DeviceIdType.MESH
BF16 = jnp.bfloat16
F32 = jnp.float32


def sin_cos(angle):
    k = jnp.floor(angle * 0.6366197723675814 + 0.5)
    r = ((angle - k * 1.5703125) - k * 4.837512969970703125e-4) - k * 7.54978995489188216e-8
    z = r * r
    sn = r + r * z * (-1.6666654611e-1 + z * (8.3321608736e-3 - 1.9515295891e-4 * z))
    cs = 1.0 - 0.5 * z + z * z * (4.166664568298827e-2 + z * (-1.388731625493765e-3 + z * 2.443315711809948e-5))
    quad = k.astype(jnp.int32)
    odd = (quad & 1) == 1
    sin = jnp.where(odd, cs, sn)
    cos = jnp.where(odd, sn, cs)
    sin = jnp.where((quad & 2) == 2, -sin, sin)
    cos = jnp.where(((quad + 1) & 2) == 2, -cos, cos)
    return sin, cos


def layer_kernel(hid_hbm, pos_hbm, gain_hbm, freq_hbm, wq_hbm, wk_hbm, wv_hbm, wg_hbm, wu_hbm, wd_hbm, wo_hbm,
                 out_hbm, kc_hbm, vc_hbm,
                 kvbuf, qbuf, acc, mbuf, lbuf, hid, h, pos, gain, freq, cost, sint,
                 wq, wk, wv, wg, wu, wd, wo, wide, kc, vc,
                 mpart, mrs1, msum, mrs2, obuf, orecv, orelay, out,
                 load_sem, hid_sem, kvs_sem, kvr_sem, dds_sem, ddr_sem, es_sem, er_sem, ys_sem, yr_sem, out_sem):
    cp = lax.axis_index('cp')
    y = lax.axis_index('tp')
    x = cp // 2
    c = cp % 2
    partner = 2 * x + 1 - c
    right = ((x + 1) % 4) * 2 + c
    left = ((x + 3) % 4) * 2 + c
    y1 = y + 1 - 2 * (y % 2)
    y2 = 3 - y
    rows = hid_hbm.shape[0]
    sub = 256
    blocks = rows // sub
    straight = 2
    quarter = sub // 4

    barrier = pltpu.get_barrier_semaphore()
    for dev in ({'cp': partner}, {'cp': right}, {'cp': left}, {'tp': y1}, {'tp': y2},
                {'tp': y1, 'cp': partner}, {'tp': y2, 'cp': partner}, {'tp': 3 - y1}, {'tp': 3 - y1, 'cp': partner}):
        pl.semaphore_signal(barrier, inc=1, device_id=dev, device_id_type=MESH)

    pairs = ((hid_hbm, hid), (pos_hbm, pos), (gain_hbm, gain), (freq_hbm, freq), (wk_hbm, wk), (wv_hbm, wv), (wq_hbm, wq),
             (wg_hbm, wg), (wu_hbm, wu), (wd_hbm, wd), (wo_hbm, wo.at[y]))
    loads = [pltpu.make_async_copy(src, dst, load_sem.at[i]) for i, (src, dst) in enumerate(pairs)]
    def hid_tile(i):
        rs = pl.ds(pl.multiple_of(i * sub, sub), sub)
        return pltpu.make_async_copy(hid_hbm.at[rs], hid.at[rs], hid_sem.at[i])

    loads[1].start()
    loads[3].start()
    hid_tile(0).start()
    for i in (2, 4, 5):
        loads[i].start()
    for i in range(1, blocks):
        hid_tile(i).start()
    for i in (6, 10):
        loads[i].start()

    def remote(src, dst, ss, rsem, dev):
        return pltpu.make_async_remote_copy(src_ref=src, dst_ref=dst, send_sem=ss, recv_sem=rsem,
                                            device_id=dev, device_id_type=MESH)

    def dd_kv(ch):
        return remote(kvbuf.at[spare], kvbuf.at[ch], dds_sem.at[0], ddr_sem.at[0], {'cp': partner})

    def dd_q(half):
        return remote(qbuf.at[2], qbuf.at[half], dds_sem.at[0], ddr_sem.at[1], {'cp': partner})

    def bytes_of(ref, ss, rsem):
        return remote(ref, ref, ss, rsem, {'cp': partner})

    class KvCopy:
        def __init__(self, ch, slot, dev):
            self.parts = []
            for p in range(2):
                ref = kvbuf.at[ch, :, pl.ds(p * (rows // 2), rows // 2)]
                self.parts.append(remote(ref, ref, kvs_sem.at[0], kvr_sem.at[ch], {'cp': dev}))
            self.whole = bytes_of(kvbuf.at[ch], kvs_sem.at[0], kvr_sem.at[ch])

        def start(self):
            for part in self.parts:
                part.start()

        def wait_recv(self):
            self.whole.wait_recv()

    kv_copy = KvCopy

    first = (y1, y2)
    second = (y2, y1)
    far = 3 - y1

    def e_copy(src, dst, i, dev):
        return remote(src, dst, es_sem.at[0], er_sem.at[i], dev)

    w_half = 2 * HEAD_DIM

    def wo_rows(shard, lo, size):
        return wo.at[shard, pl.ds(pl.multiple_of(c * w_half + lo, HEAD_DIM), size)]

    def wo_direct(i, shard):
        ref = wo_rows(shard, 0, w_half)
        return e_copy(ref, ref, i, {'tp': first[i]})

    def wo_relay(hf, shard):
        ref = wo_rows(shard, hf * HEAD_DIM, HEAD_DIM)
        return e_copy(ref, ref, 2, {'tp': first[hf]})

    def wo_partner(i):
        ref = wo_rows((y1, y2, far)[i], 0, w_half)
        return e_copy(ref, ref, 3, {'cp': partner})

    def mlp_rs1(hf, slot):
        dev = first[hf]
        beyond = (3 - dev) if hf == 0 else (dev + 1 - 2 * (dev % 2))
        tile = dev if slot == 0 else beyond
        return e_copy(mpart.at[tile, hf], mrs1.at[hf, slot], 4 + (hf if slot else 2), {'tp': dev})

    def mlp_rs2(hf):
        return e_copy(msum.at[hf], mrs2.at[hf], 7, {'tp': second[hf]})

    own_ch = 2 * x + c
    spare = kvbuf.shape[0] - 1
    oth_ch = 2 * x + 1 - c

    loads[1].wait()
    loads[3].wait()
    lane = lax.broadcasted_iota(jnp.int32, (HEAD_DIM, HEAD_DIM), 1)
    for i in range(rows // HEAD_DIM):
        at = pl.ds(i * HEAD_DIM, HEAD_DIM)
        p = jnp.broadcast_to(pos[i:i + 1, :].astype(F32), (HEAD_DIM, HEAD_DIM)).T
        sn, cs = sin_cos(p * freq[...])
        cost[at, :] = cs
        sint[at, :] = jnp.where(lane % 2 == 0, -sn, sn)
    for i in (7, 8, 9):
        loads[i].start()
    for i in (2, 4, 5):
        loads[i].wait()

    even = lax.broadcasted_iota(jnp.int32, (sub, HEAD_DIM), 1) % 2 == 0
    gain_f = gain[...].astype(F32)
    gain_row = jnp.concatenate([gain_f[i:i + 1, :] for i in range(gain.shape[0])], axis=1)

    def rope(col, rs):
        u = col.astype(BF16).astype(F32)
        swapped = jnp.where(even, pltpu.roll(u, HEAD_DIM - 1, 1), pltpu.roll(u, 1, 1))
        return (u * cost[rs, :] + swapped * sint[rs, :]).astype(BF16)

    def project_kv(i, carry):
        rs = pl.ds(pl.multiple_of(i * sub, sub), sub)
        hid_tile(i).wait()
        xx = hid[rs, :].astype(F32)
        cent = xx - jnp.mean(xx, axis=-1, keepdims=True)
        var = jnp.mean(cent * cent, axis=-1, keepdims=True)
        hh = (cent * lax.rsqrt(var + LN_EPS) * gain_row).astype(BF16)
        h[rs, :] = hh
        k = jnp.dot(hh, wk[...], preferred_element_type=F32)
        v = jnp.dot(hh, wv[...], preferred_element_type=F32).astype(BF16)
        kk = [rope(k[:, g * HEAD_DIM:(g + 1) * HEAD_DIM], rs) for g in range(2)]
        vv = [v[:, g * HEAD_DIM:(g + 1) * HEAD_DIM] for g in range(2)]
        pair_rows = pl.ds(pl.multiple_of(i * 2 * sub, 2 * sub), 2 * sub)
        for slot, (vals, out) in enumerate(((kk, kc), (vv, vc))):
            for g in range(2):
                wide[slot, pl.ds(g, sub, 2), :] = vals[g].astype(F32)
            out[pair_rows, :] = wide[slot].astype(BF16)

        for g in range(2):
            to = jnp.where(c == g, own_ch, spare)
            kvbuf[to, 0, rs, :] = kk[g]
            kvbuf[to, 1, rs, :] = vv[g]
        return carry

    def send_own(p):
        @pl.when(x < 3)
        def _():
            kv_copy(own_ch, 0, right).parts[p].start()

        @pl.when(x < 2)
        def _():
            kv_copy(own_ch, 1, left).parts[p].start()

    with jax.named_scope('kvproj'):
        lax.fori_loop(0, blocks // 2, project_kv, 0)
    with jax.named_scope('bar'):
        pl.semaphore_wait(barrier, 9)
    send_own(0)
    with jax.named_scope('kvproj'):
        lax.fori_loop(blocks // 2, blocks, project_kv, 0)
    send_own(1)
    dd_kv(own_ch).start()

    loads[10].wait()
    for i in range(2):
        wo_direct(i, y).start()

    caches = (pltpu.make_async_copy(kc, kc_hbm, load_sem.at[11]), pltpu.make_async_copy(vc, vc_hbm, load_sem.at[12]))
    for cpy in caches:
        cpy.start()
    loads[6].wait()

    def project_q(i, carry):
        rs = pl.ds(pl.multiple_of(i * sub, sub), sub)
        q = jnp.dot(h[rs, :], wq[...], preferred_element_type=F32)
        for g in range(2):
            for j in range(2):
                lo = (2 * g + j) * HEAD_DIM
                qr = rope(q[:, lo:lo + HEAD_DIM], rs)

                qbuf[jnp.where(c == g, c, 2), j, rs, :] = qr
        return carry

    with jax.named_scope('qproj'):
        lax.fori_loop(0, rows // sub, project_q, 0)
    dd_q(c).start()
    dd_kv(oth_ch).wait_recv()

    @pl.when(x < 3)
    def _():
        kv_copy(oth_ch, 2, right).start()

    @pl.when(x == 0)
    def _():
        kv_copy(oth_ch, 3, left).start()

    loads[7].wait()
    loads[8].wait()
    loads[9].wait()

    cols = (0, 512)

    def mlp(i, carry):
        rs = pl.ds(pl.multiple_of(i * sub, sub), sub)
        hh = h[rs, :]
        gate = jnp.dot(hh, wg[...], preferred_element_type=F32).astype(BF16).astype(F32)
        up = jnp.dot(hh, wu[...], preferred_element_type=F32).astype(BF16).astype(F32)
        a = (gate * (1.0 / (1.0 + jnp.exp(-gate))) * up).astype(BF16)
        tot = jnp.dot(a, wd[...], preferred_element_type=F32).astype(BF16)
        for j in range(4):
            for hf in range(2):
                mpart[j, hf, i] = tot[j * quarter:(j + 1) * quarter, cols[hf]:cols[hf] + 512]
        return carry

    with jax.named_scope('mlp'):
        lax.fori_loop(0, rows // sub, mlp, 0)

    for slot in (1, 0):
        for hf in range(2):
            mlp_rs1(hf, slot).start()
    dd_q(1 - c).wait_recv()

    def lane_sum(p):
        s = p[:, :HEAD_DIM]
        for j in range(1, p.shape[1] // HEAD_DIM):
            s = s + p[:, j * HEAD_DIM:(j + 1) * HEAD_DIM]
        return s

    def qk(qv, kv):
        return lax.dot_general(qv, kv, (((1,), (1,)), ((), ())), preferred_element_type=F32)

    k0, k1, v0, v1 = (kvbuf.at[2 * x, 0], kvbuf.at[2 * x + 1, 0], kvbuf.at[2 * x, 1], kvbuf.at[2 * x + 1, 1])
    tri = (lax.broadcasted_iota(jnp.int32, (sub, sub), 1) <= lax.broadcasted_iota(jnp.int32, (sub, sub), 0))
    groups = rows // sub

    def diag_scores(r, g):
        half, off = r // groups, (r % groups) * sub
        qv = qbuf[half, g, pl.ds(off, sub), :]
        pieces = []
        if half == 1:
            pieces.append(qk(qv, k0[...]))
        kk = k0 if half == 0 else k1
        if off:
            pieces.append(qk(qv, kk[pl.ds(0, off), :]))
        pieces.append(jnp.where(tri, qk(qv, kk[pl.ds(off, sub), :]), -jnp.inf))
        return pieces[0] if len(pieces) == 1 else jnp.concatenate(pieces, axis=1)

    def diag_soft(r, g, s):
        half, off = r // groups, (r % groups) * sub
        rs = pl.ds(off, sub)
        mx = jnp.max(s, axis=1, keepdims=True)
        p = jnp.exp2((s - mx) * EXP2_SCALE)
        pb = p.astype(BF16)
        if half == 0:
            o = jnp.dot(pb, v0[pl.ds(0, off + sub), :], preferred_element_type=F32)
        else:
            o = jnp.dot(pb[:, :rows], v0[...], preferred_element_type=F32)
            o = o + jnp.dot(pb[:, rows:], v1[pl.ds(0, off + sub), :], preferred_element_type=F32)
        mbuf[g, half, rs, :] = jnp.broadcast_to(mx, (sub, HEAD_DIM))
        lbuf[g, half, rs, :] = lane_sum(p)
        acc[g, half, rs, :] = o

    items = [(r, g) for r in range(2 * groups) for g in range(2)]
    own_block = jax.named_scope('diag')
    own_block.__enter__()
    s_now = diag_scores(*items[0])
    for i, it in enumerate(items):
        s_next = diag_scores(*items[i + 1]) if i + 1 < len(items) else None
        diag_soft(*it, s_now)
        s_now = s_next

    own_block.__exit__(None, None, None)
    for hf in range(2):
        wo_direct(1 - hf, second[hf]).wait_recv()
        wo_relay(hf, second[hf]).start()

    @pl.when(x == 0)
    def _():
        kv_copy(2 + c, 0, right).wait_recv()
        kv_copy(2 + c, 4, left).start()

    def attend(chunks, its):
        def scores(it):
            g, half, rs = it
            qv = qbuf[half, g, rs, :]
            pieces = [qk(qv, kvbuf[ch, 0]) for ch in chunks]
            return pieces[0] if len(pieces) == 1 else jnp.concatenate(pieces, axis=1)

        s = scores(its[0])
        for i, it in enumerate(its):
            s_n = scores(its[i + 1]) if i + 1 < len(its) else None
            g, half, rs = it
            m_old = mbuf[g, half, rs, :]
            m_new = jnp.maximum(m_old, jnp.max(s, axis=1, keepdims=True))
            alpha = jnp.exp2((m_old - m_new) * EXP2_SCALE)
            p = jnp.exp2((s - m_new[:, :1]) * EXP2_SCALE)
            lbuf[g, half, rs, :] = lbuf[g, half, rs, :] * alpha + lane_sum(p)
            pb = p.astype(BF16)
            o = acc[g, half, rs, :] * alpha
            for i_ch, ch in enumerate(chunks):
                o = o + jnp.dot(pb[:, i_ch * rows:(i_ch + 1) * rows], kvbuf[ch, 1], preferred_element_type=F32)
            acc[g, half, rs, :] = o
            mbuf[g, half, rs, :] = m_new
            s = s_n

    def block_rows(b):
        return pl.ds(pl.multiple_of(b * sub, sub), sub)

    def attend_pair(ch_a, ch_b, pair):
        attend((ch_a, ch_b), [(g, half, block_rows(2 * pair + j)) for half in range(2) for j in range(2) for g in range(2)])

    def attend_last(ch_a, ch_b, b):
        attend((ch_a, ch_b), [(g, half, block_rows(b)) for half in range(2) for g in range(2)])

    def y_copy(src, dst, b, i, dev):
        return remote(src, dst, ys_sem.at[b], yr_sem.at[b, i], dev)

    def o_direct(b, i, core):
        return remote(obuf.at[b, first[i], core], orecv.at[b, y, c], ys_sem.at[b], yr_sem.at[b, 0],
                      {'tp': first[i], 'cp': 2 * x + core})

    def o_far(b, hf, core):
        return remote(obuf.at[b, far, core, hf], orelay.at[b, hf, c], ys_sem.at[b], yr_sem.at[b, 1],
                      {'tp': first[hf], 'cp': 2 * x + core})

    def o_relay(b, hf):
        return y_copy(orelay.at[b, hf], orecv.at[b, first[hf], :, hf], b, 0, {'tp': second[hf]})

    def o_beyond(b, core):
        return remote(obuf.at[b, far, core], orecv.at[b, y, c], ys_sem.at[b], yr_sem.at[b, 0],
                      {'tp': far, 'cp': 2 * x + core})

    def o_partner(b):
        return y_copy(obuf.at[b, y, 1 - c], orecv.at[b, y, c], b, 0, {'cp': partner})

    def xt(b, t, hf):
        return out.at[pl.ds(pl.multiple_of(b * sub + t * quarter, quarter), quarter), pl.ds(cols[hf], 512)]

    def ag1_copy(b, hf):
        return y_copy(xt(b, y, hf), xt(b, y, hf), b, 2 + hf, {'tp': second[hf]})

    def ag1_wait(b, hf):
        t = second[hf]
        y_copy(xt(b, t, hf), xt(b, t, hf), b, 2 + hf, {'tp': t}).wait_recv()

    def ag2_copy(b, hf, slot):
        t = y if slot == 0 else second[hf]
        return y_copy(xt(b, t, hf), xt(b, t, hf), b, 4, {'tp': first[hf]})

    def finish(b):
        rs = block_rows(b)
        for half in range(2):
            for g in range(2):
                den = jnp.sum(lbuf[g, half, rs, :], axis=1, keepdims=True)
                o = (acc[g, half, rs, :] / den).astype(BF16)
                for j in range(4):
                    obuf[b, j, half, g] = o[j * quarter:(j + 1) * quarter, :]
        @pl.when(b < straight)
        def _():
            for hf in range(2):
                for core in range(2):
                    o_far(b, hf, core).start()

        @pl.when(b >= straight)
        def _():
            for core in range(2):
                o_beyond(b, core).start()

        for i in range(2):
            for core in range(2):
                o_direct(b, i, core).start()
        o_partner(b).start()
        orecv[b, y, c] = obuf[b, y, c]

    def step1(b):
        @pl.when(b < straight)
        def _():
            bytes_of(orelay.at[b], ys_sem.at[b], yr_sem.at[b, 1]).wait_recv()
            for hf in range(2):
                o_relay(b, hf).start()

    def step2(b):
        own_rows = pl.ds(pl.multiple_of(b * sub + y * quarter, quarter), quarter)

        @pl.when(b == 0)
        def _():
            bytes_of(wo.at[pl.ds(0, 3), pl.ds(0, w_half)], es_sem.at[0], er_sem.at[3]).wait_recv()
            bytes_of(mrs1.at[:, 0], es_sem.at[0], er_sem.at[6]).wait_recv()
            bytes_of(mrs2, es_sem.at[0], er_sem.at[7]).wait_recv()

        bytes_of(hid.at[pl.ds(0, 7 * quarter // 4)], ys_sem.at[b], yr_sem.at[b, 0]).wait_recv()
        lhs = jnp.concatenate([orecv[b, src, core, g] for src in range(4) for core in range(2) for g in range(2)], axis=1)
        attn = jnp.dot(lhs, jnp.concatenate([wo[src] for src in range(4)], axis=0), preferred_element_type=F32)
        for hf in range(2):
            at = slice(cols[hf], cols[hf] + 512)
            mlp_tot = mpart[y, hf, b].astype(F32) + mrs1[hf, 0, b].astype(F32) + mrs2[hf, b].astype(F32)
            out[own_rows, at] = (hid[own_rows, at].astype(F32) + attn[:, at] + mlp_tot).astype(BF16)
            ag1_copy(b, hf).start()
        for hf in range(2):
            ag2_copy(b, hf, 0).start()

    def early_sends():
        for cpy in caches:
            cpy.wait()
        for i in range(4):
            @pl.when(x == i)
            def _():
                bytes_of(kvbuf.at[pl.ds(0, (5, 4, 3, 1)[i])], kvs_sem.at[0], kvr_sem.at[0]).wait_send()

        bytes_of(kvbuf.at[pl.ds(0, 2)], dds_sem.at[0], ddr_sem.at[0]).wait_send()
        bytes_of(kvbuf.at[pl.ds(0, 9)], es_sem.at[0], er_sem.at[0]).wait_send()

    def step3(b):
        @pl.when(b == blocks - 1)
        def _():
            early_sends()

        for hf in range(2):
            ag1_wait(b, hf)
            ag2_copy(b, hf, 1).start()

    def out_copy(b):
        return pltpu.make_async_copy(out.at[block_rows(b)], out_hbm.at[block_rows(b)], out_sem.at[0])

    def step4(b):
        bytes_of(hid.at[pl.ds(0, 2 * quarter)], ys_sem.at[b], yr_sem.at[b, 4]).wait_recv()
        out_copy(b).start()

    n = 2 * x

    def chunk_of(s):
        first_half = s // 2
        par = s % 2
        near = 2 * (x - 1 - first_half) + (c + par - 2 * c * par)
        mix_half = c + first_half - 2 * c * first_half
        mixed = 4 - 4 * par + mix_half
        late = 2 + (c + par - 2 * c * par)
        three = jnp.where(s < 4, mixed, late)
        return jnp.where(x == 3, three, near)

    three = x == 3
    lead = 2 * (x // 2) + x // 3
    ticks = lead + 8 + 2 * (x // 3)

    def pick(tau, near, far):
        b = jnp.int32(-1)
        for i in range(4):
            b = jnp.where(tau == jnp.where(three, far[i], near[i]), i, b)
        return jnp.maximum(b, 0), b >= 0

    def loop(t, carry):
        tau = t - lead
        gap = jnp.logical_and(three, jnp.logical_or(tau == 0, tau == 3))
        s = jnp.where(t == 2, 2, 0)
        pair = jnp.where(t == 1, 1, 0)

        @pl.when(jnp.logical_and(tau < 0, t != 1))
        def _():
            ch_b = chunk_of(s + 1)
            kv_copy(ch_b, 0, right).wait_recv()

            @pl.when(jnp.logical_and(three, t == 0))
            def _():
                kv_copy(ch_b, 0, left).start()

            @pl.when(x == 2)
            def _():
                kv_copy(ch_b, 1, right).start()

            kv_copy(chunk_of(s), 0, right).wait_recv()

        @pl.when(jnp.logical_and(x > 0, tau == x // 3))
        def _():
            kv_copy(chunk_of(n - 2), 0, right).wait_recv()
            kv_copy(chunk_of(n - 1), 0, right).wait_recv()

            @pl.when(x == 1)
            def _():
                kv_copy(chunk_of(1), 3, right).start()

        @pl.when(t == (x // 2) * (x - 1))
        def _():
            with jax.named_scope('e2'):
                for hf in range(2):
                    mlp_rs1(hf, 1).wait_recv()
                    msum[hf] = (mpart[second[hf], hf].astype(F32) + mrs1[hf, 1].astype(F32)).astype(BF16)
                    mlp_rs2(hf).start()

        @pl.when(tau == x // 3)
        def _():
            with jax.named_scope('e3'):
                bytes_of(wo.at[far, pl.ds(0, w_half)], es_sem.at[0], er_sem.at[2]).wait_recv()
                for i in range(3):
                    wo_partner(i).start()

        @pl.when(tau < 0)
        def _():
            with jax.named_scope('att'):
                attend_pair(chunk_of(s), chunk_of(s + 1), pair)

        b0, ok0 = pick(tau, (0, 1, 2, 3), (1, 2, 4, 5))

        @pl.when(jnp.logical_and(jnp.logical_or(ok0, gap), x > 0))
        def _():
            back = jnp.where(gap, 4, 2)
            with jax.named_scope('last'):
                attend_last(chunk_of(n - back), chunk_of(n - back + 1), jnp.where(gap, 2 + tau // 3, b0))

        def service(fn, nm, near_t, far_t):
            bk, okk = pick(tau, near_t, far_t)

            @pl.when(okk)
            def _():
                with jax.named_scope(nm):
                    fn(bk)

        service(step3, 's3', (4, 5, 6, 7), (5, 6, 8, 9))
        service(step1, 's1', (1, 2, 3, 4), (2, 3, 5, 6))

        @pl.when(ok0)
        def _():
            with jax.named_scope('finish'):
                finish(b0)

        service(step2, 's2', (2, 3, 4, 5), (3, 4, 5, 7))
        return carry

    lax.fori_loop(0, ticks, loop, 0)

    def last_step(b, carry):
        with jax.named_scope('s4'):
            step4(b)
        return carry

    lax.fori_loop(0, blocks, last_step, 0)

    for b in range(blocks):
        pieces = 7 + 12 + (2 if b < straight else 0)
        bytes_of(hid.at[pl.ds(0, pieces * quarter // 4)], ys_sem.at[b], yr_sem.at[b, 0]).wait_send()
    pltpu.make_async_copy(out, out_hbm, out_sem.at[0]).wait()


def layer(hidden, positions, gain, w_q, w_k, w_v, w_gate, w_up, w_down, w_o):
    rows, width = hidden.shape
    ff = w_gate.shape[1]
    hr = 256
    nb = rows // hr
    qr = hr // 4
    hw = width // 2
    freq = 1.0 / (ROPE_BASE ** (np.repeat(np.arange(0, HEAD_DIM, 2), 2) / HEAD_DIM))
    freq = jnp.asarray(freq[None, :], F32)
    anyspec = pl.BlockSpec(memory_space=pl.ANY)
    vm = pltpu.VMEM
    dma = pltpu.SemaphoreType.DMA
    return pl.pallas_call(
        layer_kernel,
        in_specs=[anyspec] * 11,
        out_specs=[anyspec] * 3,
        out_shape=[jax.ShapeDtypeStruct((rows, width), BF16),
                   jax.ShapeDtypeStruct((rows * w_k.shape[1] // HEAD_DIM, HEAD_DIM), BF16),
                   jax.ShapeDtypeStruct((rows * w_v.shape[1] // HEAD_DIM, HEAD_DIM), BF16)],
        scratch_shapes=[
            vm((9, 2, rows, HEAD_DIM), BF16),
            vm((3, 2, rows, HEAD_DIM), BF16),
            vm((2, 2, rows, HEAD_DIM), F32),
            vm((2, 2, rows, HEAD_DIM), F32),
            vm((2, 2, rows, HEAD_DIM), F32),
            vm((rows, width), BF16),
            vm((rows, width), BF16),
            vm((rows // HEAD_DIM, HEAD_DIM), jnp.int32),
            vm((width // HEAD_DIM, HEAD_DIM), BF16),
            vm((1, HEAD_DIM), F32),
            vm((rows, HEAD_DIM), F32),
            vm((rows, HEAD_DIM), F32),
            vm(w_q.shape, BF16), vm(w_k.shape, BF16), vm(w_v.shape, BF16),
            vm((width, ff), BF16), vm((width, ff), BF16), vm((ff, width), BF16),
            vm((4,) + w_o.shape, BF16),
            vm((2, 2 * hr, HEAD_DIM), F32),
            vm((rows * w_k.shape[1] // HEAD_DIM, HEAD_DIM), BF16),
            vm((rows * w_v.shape[1] // HEAD_DIM, HEAD_DIM), BF16),
            vm((4, 2, nb, qr, hw), BF16),
            vm((2, 2, nb, qr, hw), BF16),
            vm((2, nb, qr, hw), BF16),
            vm((2, nb, qr, hw), BF16),
            vm((nb, 4, 2, 2, qr, HEAD_DIM), BF16),
            vm((nb, 4, 2, 2, qr, HEAD_DIM), BF16),
            vm((nb, 2, 2, qr, HEAD_DIM), BF16),
            vm((rows, width), BF16),
            dma((13,)), dma((nb,)), dma((1,)), dma((8,)), dma((1,)), dma((2,)), dma((1,)), dma((8,)),
            dma((nb,)), dma((nb, 5)), dma((1,)),
        ],
        compiler_params=pltpu.CompilerParams(collective_id=0, has_side_effects=True, vmem_limit_bytes=62 << 20),
        name='layer',
    )(hidden, positions.reshape(rows // HEAD_DIM, HEAD_DIM), gain.reshape(width // HEAD_DIM, HEAD_DIM), freq,
      w_q, w_k, w_v, w_gate, w_up, w_down, w_o)


def solution(mesh):
    def local_layer(hidden, positions, ln_gain, w_q, w_k, w_v, w_o, w_gate, w_up, w_down):
        rows = hidden.shape[0]
        kv_local = w_k.shape[1] // HEAD_DIM
        out, kc, vc = layer(hidden, positions, ln_gain, w_q, w_k, w_v, w_gate, w_up, w_down, w_o)
        return out, kc.reshape(rows, kv_local, HEAD_DIM), vc.reshape(rows, kv_local, HEAD_DIM)

    row_spec = P(('dp', 'cp'), None)
    col_spec = P(None, 'tp')
    cache_spec = P(('dp', 'cp'), 'tp', None)
    in_specs = (row_spec, P(('dp', 'cp')), P(None), col_spec, col_spec, col_spec, P('tp', None), col_spec, col_spec, P('tp', None))
    return jax.shard_map(local_layer, mesh=mesh, in_specs=in_specs, out_specs=(row_spec, cache_spec, cache_spec), check_vma=False)
```

```python
import jax
import jax.numpy as jnp
import numpy as np
from jax import lax
from jax.experimental import pallas as pl
from jax.experimental.pallas import tpu as pltpu
from jax.sharding import PartitionSpec as P

HEAD_DIM = 128
ROPE_BASE = 4000000
LN_EPS = 1e-5
EXP2_SCALE = (HEAD_DIM ** -0.5) * 1.4426950408889634
MESH = pl.DeviceIdType.MESH
BF16 = jnp.bfloat16
F32 = jnp.float32


def sin_cos(angle):
    k = jnp.floor(angle * 0.6366197723675814 + 0.5)
    r = ((angle - k * 1.5703125) - k * 4.837512969970703125e-4) - k * 7.54978995489188216e-8
    z = r * r
    sn = r + r * z * (-1.6666654611e-1 + z * (8.3321608736e-3 - 1.9515295891e-4 * z))
    cs = 1.0 - 0.5 * z + z * z * (4.166664568298827e-2 + z * (-1.388731625493765e-3 + z * 2.443315711809948e-5))
    quad = k.astype(jnp.int32)
    odd = (quad & 1) == 1
    sin = jnp.where(odd, cs, sn)
    cos = jnp.where(odd, sn, cs)
    sin = jnp.where((quad & 2) == 2, -sin, sin)
    cos = jnp.where(((quad + 1) & 2) == 2, -cos, cos)
    return sin, cos


def layer_kernel(hid_hbm, pos_hbm, gain_hbm, freq_hbm, wq_hbm, wk_hbm, wv_hbm, wg_hbm, wu_hbm, wd_hbm, wo_hbm,
                 out_hbm, kc_hbm, vc_hbm,
                 kvbuf, qbuf, acc, mbuf, lbuf, hid, h, pos, gain, freq, cost, sint,
                 wq, wk, wv, wg, wu, wd, wo, wide, kc, vc,
                 mpart, mrs1, msum, mrs2, obuf, orecv, orelay, out,
                 load_sem, hid_sem, kvs_sem, kvr_sem, dds_sem, ddr_sem, es_sem, er_sem, ys_sem, yr_sem, out_sem):
    cp = lax.axis_index('cp')
    y = lax.axis_index('tp')
    x = cp // 2
    c = cp % 2
    partner = 2 * x + 1 - c
    right = ((x + 1) % 4) * 2 + c
    left = ((x + 3) % 4) * 2 + c
    y1 = y + 1 - 2 * (y % 2)
    y2 = 3 - y
    rows = hid_hbm.shape[0]
    sub = 256
    blocks = rows // sub
    straight = 2
    quarter = sub // 4

    barrier = pltpu.get_barrier_semaphore()
    for dev in ({'cp': partner}, {'cp': right}, {'cp': left}, {'tp': y1}, {'tp': y2},
                {'tp': y1, 'cp': partner}, {'tp': y2, 'cp': partner}, {'tp': 3 - y1}, {'tp': 3 - y1, 'cp': partner}):
        pl.semaphore_signal(barrier, inc=1, device_id=dev, device_id_type=MESH)

    pairs = ((hid_hbm, hid), (pos_hbm, pos), (gain_hbm, gain), (freq_hbm, freq), (wk_hbm, wk), (wv_hbm, wv), (wq_hbm, wq),
             (wg_hbm, wg), (wu_hbm, wu), (wd_hbm, wd), (wo_hbm, wo.at[y]))
    loads = [pltpu.make_async_copy(src, dst, load_sem.at[i]) for i, (src, dst) in enumerate(pairs)]
    def hid_tile(i):
        rs = pl.ds(pl.multiple_of(i * sub, sub), sub)
        return pltpu.make_async_copy(hid_hbm.at[rs], hid.at[rs], hid_sem.at[i])

    loads[1].start()
    loads[3].start()
    hid_tile(0).start()
    for i in (2, 4, 5):
        loads[i].start()
    for i in range(1, blocks):
        hid_tile(i).start()
    for i in (6, 10):
        loads[i].start()

    def remote(src, dst, ss, rsem, dev):
        return pltpu.make_async_remote_copy(src_ref=src, dst_ref=dst, send_sem=ss, recv_sem=rsem,
                                            device_id=dev, device_id_type=MESH)

    def dd_kv(ch):
        return remote(kvbuf.at[spare], kvbuf.at[ch], dds_sem.at[0], ddr_sem.at[0], {'cp': partner})

    def dd_q(half):
        return remote(qbuf.at[2], qbuf.at[half], dds_sem.at[0], ddr_sem.at[1], {'cp': partner})

    def bytes_of(ref, ss, rsem):
        return remote(ref, ref, ss, rsem, {'cp': partner})

    class KvCopy:
        def __init__(self, ch, slot, dev):
            self.parts = []
            for p in range(2):
                ref = kvbuf.at[ch, :, pl.ds(p * (rows // 2), rows // 2)]
                self.parts.append(remote(ref, ref, kvs_sem.at[0], kvr_sem.at[ch], {'cp': dev}))
            self.whole = bytes_of(kvbuf.at[ch], kvs_sem.at[0], kvr_sem.at[ch])

        def start(self):
            for part in self.parts:
                part.start()

        def wait_recv(self):
            self.whole.wait_recv()

    kv_copy = KvCopy

    first = (y1, y2)
    second = (y2, y1)
    far = 3 - y1

    def e_copy(src, dst, i, dev):
        return remote(src, dst, es_sem.at[0], er_sem.at[i], dev)

    w_half = 2 * HEAD_DIM

    def wo_rows(shard, lo, size):
        return wo.at[shard, pl.ds(pl.multiple_of(c * w_half + lo, HEAD_DIM), size)]

    def wo_direct(i, shard):
        ref = wo_rows(shard, 0, w_half)
        return e_copy(ref, ref, i, {'tp': first[i]})

    def wo_relay(hf, shard):
        ref = wo_rows(shard, hf * HEAD_DIM, HEAD_DIM)
        return e_copy(ref, ref, 2, {'tp': first[hf]})

    def wo_partner(i):
        ref = wo_rows((y1, y2, far)[i], 0, w_half)
        return e_copy(ref, ref, 3, {'cp': partner})

    def mlp_rs1(hf, slot):
        dev = first[hf]
        beyond = (3 - dev) if hf == 0 else (dev + 1 - 2 * (dev % 2))
        tile = dev if slot == 0 else beyond
        return e_copy(mpart.at[tile, hf], mrs1.at[hf, slot], 4 + (hf if slot else 2), {'tp': dev})

    def mlp_rs2(hf):
        return e_copy(msum.at[hf], mrs2.at[hf], 7, {'tp': second[hf]})

    own_ch = 2 * x + c
    spare = kvbuf.shape[0] - 1
    oth_ch = 2 * x + 1 - c

    loads[1].wait()
    loads[3].wait()
    lane = lax.broadcasted_iota(jnp.int32, (HEAD_DIM, HEAD_DIM), 1)
    for i in range(rows // HEAD_DIM):
        at = pl.ds(i * HEAD_DIM, HEAD_DIM)
        p = jnp.broadcast_to(pos[i:i + 1, :].astype(F32), (HEAD_DIM, HEAD_DIM)).T
        sn, cs = sin_cos(p * freq[...])
        cost[at, :] = cs
        sint[at, :] = jnp.where(lane % 2 == 0, -sn, sn)
    for i in (7, 8, 9):
        loads[i].start()
    for i in (2, 4, 5):
        loads[i].wait()

    gain_f = gain[...].astype(F32)
    gain_row = jnp.concatenate([gain_f[i:i + 1, :] for i in range(gain.shape[0])], axis=1)

    def rope(col, rs):
        u = col.astype(BF16).astype(F32)
        even = lax.broadcasted_iota(jnp.int32, u.shape, 1) % 2 == 0
        swapped = jnp.where(even, pltpu.roll(u, HEAD_DIM - 1, 1), pltpu.roll(u, 1, 1))
        return (u * cost[rs, :] + swapped * sint[rs, :]).astype(BF16)

    def project_kv(i, carry):
        rs = pl.ds(pl.multiple_of(i * sub, sub), sub)
        hid_tile(i).wait()
        xx = hid[rs, :].astype(F32)
        cent = xx - jnp.mean(xx, axis=-1, keepdims=True)
        var = jnp.mean(cent * cent, axis=-1, keepdims=True)
        hh = (cent * lax.rsqrt(var + LN_EPS) * gain_row).astype(BF16)
        h[rs, :] = hh
        k = jnp.dot(hh, wk[...], preferred_element_type=F32)
        v = jnp.dot(hh, wv[...], preferred_element_type=F32).astype(BF16)
        kk = [rope(k[:, g * HEAD_DIM:(g + 1) * HEAD_DIM], rs) for g in range(2)]
        vv = [v[:, g * HEAD_DIM:(g + 1) * HEAD_DIM] for g in range(2)]
        pair_rows = pl.ds(pl.multiple_of(i * 2 * sub, 2 * sub), 2 * sub)
        for slot, (vals, out) in enumerate(((kk, kc), (vv, vc))):
            for g in range(2):
                wide[slot, pl.ds(g, sub, 2), :] = vals[g].astype(F32)
            out[pair_rows, :] = wide[slot].astype(BF16)

        for g in range(2):
            to = jnp.where(c == g, own_ch, spare)
            kvbuf[to, 0, rs, :] = kk[g]
            kvbuf[to, 1, rs, :] = vv[g]
        return carry

    def send_own(p):
        @pl.when(x < 3)
        def _():
            kv_copy(own_ch, 0, right).parts[p].start()

        @pl.when(x < 2)
        def _():
            kv_copy(own_ch, 1, left).parts[p].start()

    with jax.named_scope('kvproj'):
        lax.fori_loop(0, blocks // 2, project_kv, 0)
    with jax.named_scope('bar'):
        pl.semaphore_wait(barrier, 9)
    send_own(0)
    with jax.named_scope('kvproj'):
        lax.fori_loop(blocks // 2, blocks, project_kv, 0)
    send_own(1)
    dd_kv(own_ch).start()

    loads[10].wait()
    for i in range(2):
        wo_direct(i, y).start()

    caches = (pltpu.make_async_copy(kc, kc_hbm, load_sem.at[11]), pltpu.make_async_copy(vc, vc_hbm, load_sem.at[12]))
    for cpy in caches:
        cpy.start()
    loads[6].wait()

    def project_q(i, carry):
        rs = pl.ds(pl.multiple_of(i * 2 * sub, 2 * sub), 2 * sub)
        q = jnp.dot(h[rs, :], wq[...], preferred_element_type=F32)
        for g in range(2):
            for j in range(2):
                lo = (2 * g + j) * HEAD_DIM
                qr = rope(q[:, lo:lo + HEAD_DIM], rs)

                qbuf[jnp.where(c == g, c, 2), j, rs, :] = qr
        return carry

    with jax.named_scope('qproj'):
        lax.fori_loop(0, rows // (2 * sub), project_q, 0)
    dd_q(c).start()
    dd_kv(oth_ch).wait_recv()

    @pl.when(x < 3)
    def _():
        kv_copy(oth_ch, 2, right).start()

    @pl.when(x == 0)
    def _():
        kv_copy(oth_ch, 3, left).start()

    loads[7].wait()
    loads[8].wait()
    loads[9].wait()

    cols = (0, 512)

    def mlp(i, carry):
        rs = pl.ds(pl.multiple_of(i * 2 * sub, 2 * sub), 2 * sub)
        hh = h[rs, :]
        gate = jnp.dot(hh, wg[...], preferred_element_type=F32).astype(BF16).astype(F32)
        up = jnp.dot(hh, wu[...], preferred_element_type=F32).astype(BF16).astype(F32)
        a = (gate * (1.0 / (1.0 + jnp.exp(-gate))) * up).astype(BF16)
        tot = jnp.dot(a, wd[...], preferred_element_type=F32).astype(BF16)
        for k in range(2):
            for j in range(4):
                lo = k * sub + j * quarter
                for hf in range(2):
                    mpart[j, hf, 2 * i + k] = tot[lo:lo + quarter, cols[hf]:cols[hf] + 512]
        return carry

    with jax.named_scope('mlp'):
        lax.fori_loop(0, rows // (2 * sub), mlp, 0)

    for slot in (1, 0):
        for hf in range(2):
            mlp_rs1(hf, slot).start()
    dd_q(1 - c).wait_recv()

    def lane_sum(p):
        s = p[:, :HEAD_DIM]
        for j in range(1, p.shape[1] // HEAD_DIM):
            s = s + p[:, j * HEAD_DIM:(j + 1) * HEAD_DIM]
        return s

    def qk(qv, kv):
        return lax.dot_general(qv, kv, (((1,), (1,)), ((), ())), preferred_element_type=F32)

    k0, k1, v0, v1 = (kvbuf.at[2 * x, 0], kvbuf.at[2 * x + 1, 0], kvbuf.at[2 * x, 1], kvbuf.at[2 * x + 1, 1])
    tri = (lax.broadcasted_iota(jnp.int32, (sub, sub), 1) <= lax.broadcasted_iota(jnp.int32, (sub, sub), 0))
    groups = rows // sub

    def diag_scores(r, g):
        half, off = r // groups, (r % groups) * sub
        qv = qbuf[half, g, pl.ds(off, sub), :]
        pieces = []
        if half == 1:
            pieces.append(qk(qv, k0[...]))
        kk = k0 if half == 0 else k1
        if off:
            pieces.append(qk(qv, kk[pl.ds(0, off), :]))
        pieces.append(jnp.where(tri, qk(qv, kk[pl.ds(off, sub), :]), -jnp.inf))
        return pieces[0] if len(pieces) == 1 else jnp.concatenate(pieces, axis=1)

    def diag_soft(r, g, s):
        half, off = r // groups, (r % groups) * sub
        rs = pl.ds(off, sub)
        mx = jnp.max(s, axis=1, keepdims=True)
        p = jnp.exp2((s - mx) * EXP2_SCALE)
        pb = p.astype(BF16)
        if half == 0:
            o = jnp.dot(pb, v0[pl.ds(0, off + sub), :], preferred_element_type=F32)
        else:
            o = jnp.dot(pb[:, :rows], v0[...], preferred_element_type=F32)
            o = o + jnp.dot(pb[:, rows:], v1[pl.ds(0, off + sub), :], preferred_element_type=F32)
        mbuf[g, half, rs, :] = jnp.broadcast_to(mx, (sub, HEAD_DIM))
        lbuf[g, half, rs, :] = lane_sum(p)
        acc[g, half, rs, :] = o

    items = [(r, g) for r in range(2 * groups) for g in range(2)]
    own_block = jax.named_scope('diag')
    own_block.__enter__()
    s_now = diag_scores(*items[0])
    for i, it in enumerate(items):
        s_next = diag_scores(*items[i + 1]) if i + 1 < len(items) else None
        diag_soft(*it, s_now)
        s_now = s_next

    own_block.__exit__(None, None, None)
    for hf in range(2):
        wo_direct(1 - hf, second[hf]).wait_recv()
        wo_relay(hf, second[hf]).start()

    @pl.when(x == 0)
    def _():
        kv_copy(2 + c, 0, right).wait_recv()
        kv_copy(2 + c, 4, left).start()

    def attend(chunks, its):
        def scores(it):
            g, half, rs = it
            qv = qbuf[half, g, rs, :]
            pieces = [qk(qv, kvbuf[ch, 0]) for ch in chunks]
            return pieces[0] if len(pieces) == 1 else jnp.concatenate(pieces, axis=1)

        s = scores(its[0])
        for i, it in enumerate(its):
            s_n = scores(its[i + 1]) if i + 1 < len(its) else None
            g, half, rs = it
            m_old = mbuf[g, half, rs, :]
            m_new = jnp.maximum(m_old, jnp.max(s, axis=1, keepdims=True))
            alpha = jnp.exp2((m_old - m_new) * EXP2_SCALE)
            p = jnp.exp2((s - m_new[:, :1]) * EXP2_SCALE)
            lbuf[g, half, rs, :] = lbuf[g, half, rs, :] * alpha + lane_sum(p)
            pb = p.astype(BF16)
            o = acc[g, half, rs, :] * alpha
            for i_ch, ch in enumerate(chunks):
                o = o + jnp.dot(pb[:, i_ch * rows:(i_ch + 1) * rows], kvbuf[ch, 1], preferred_element_type=F32)
            acc[g, half, rs, :] = o
            mbuf[g, half, rs, :] = m_new
            s = s_n

    def block_rows(b):
        return pl.ds(pl.multiple_of(b * sub, sub), sub)

    def attend_pair(ch_a, ch_b, pair):
        attend((ch_a, ch_b), [(g, half, block_rows(2 * pair + j)) for half in range(2) for j in range(2) for g in range(2)])

    def attend_last(ch_a, ch_b, b):
        attend((ch_a, ch_b), [(g, half, block_rows(b)) for half in range(2) for g in range(2)])

    def y_copy(src, dst, b, i, dev):
        return remote(src, dst, ys_sem.at[b], yr_sem.at[b, i], dev)

    def o_direct(b, i, core):
        return remote(obuf.at[b, first[i], core], orecv.at[b, y, c], ys_sem.at[b], yr_sem.at[b, 0],
                      {'tp': first[i], 'cp': 2 * x + core})

    def o_far(b, hf, core):
        return remote(obuf.at[b, far, core, hf], orelay.at[b, hf, c], ys_sem.at[b], yr_sem.at[b, 1],
                      {'tp': first[hf], 'cp': 2 * x + core})

    def o_relay(b, hf):
        return y_copy(orelay.at[b, hf], orecv.at[b, first[hf], :, hf], b, 0, {'tp': second[hf]})

    def o_beyond(b, core):
        return remote(obuf.at[b, far, core], orecv.at[b, y, c], ys_sem.at[b], yr_sem.at[b, 0],
                      {'tp': far, 'cp': 2 * x + core})

    def o_partner(b):
        return y_copy(obuf.at[b, y, 1 - c], orecv.at[b, y, c], b, 0, {'cp': partner})

    def xt(b, t, hf):
        return out.at[pl.ds(pl.multiple_of(b * sub + t * quarter, quarter), quarter), pl.ds(cols[hf], 512)]

    def ag1_copy(b, hf):
        return y_copy(xt(b, y, hf), xt(b, y, hf), b, 2 + hf, {'tp': second[hf]})

    def ag1_wait(b, hf):
        t = second[hf]
        y_copy(xt(b, t, hf), xt(b, t, hf), b, 2 + hf, {'tp': t}).wait_recv()

    def ag2_copy(b, hf, slot):
        t = y if slot == 0 else second[hf]
        return y_copy(xt(b, t, hf), xt(b, t, hf), b, 4, {'tp': first[hf]})

    def finish(b):
        rs = block_rows(b)
        for half in range(2):
            for g in range(2):
                den = jnp.sum(lbuf[g, half, rs, :], axis=1, keepdims=True)
                o = (acc[g, half, rs, :] / den).astype(BF16)
                for j in range(4):
                    obuf[b, j, half, g] = o[j * quarter:(j + 1) * quarter, :]
        @pl.when(b < straight)
        def _():
            for hf in range(2):
                for core in range(2):
                    o_far(b, hf, core).start()

        @pl.when(b >= straight)
        def _():
            for core in range(2):
                o_beyond(b, core).start()

        for i in range(2):
            for core in range(2):
                o_direct(b, i, core).start()
        o_partner(b).start()
        orecv[b, y, c] = obuf[b, y, c]

    def step1(b):
        @pl.when(b < straight)
        def _():
            bytes_of(orelay.at[b], ys_sem.at[b], yr_sem.at[b, 1]).wait_recv()
            for hf in range(2):
                o_relay(b, hf).start()

    def step2(b):
        own_rows = pl.ds(pl.multiple_of(b * sub + y * quarter, quarter), quarter)

        @pl.when(b == 0)
        def _():
            bytes_of(wo.at[pl.ds(0, 3), pl.ds(0, w_half)], es_sem.at[0], er_sem.at[3]).wait_recv()
            bytes_of(mrs1.at[:, 0], es_sem.at[0], er_sem.at[6]).wait_recv()
            bytes_of(mrs2, es_sem.at[0], er_sem.at[7]).wait_recv()

        bytes_of(hid.at[pl.ds(0, 7 * quarter // 4)], ys_sem.at[b], yr_sem.at[b, 0]).wait_recv()
        lhs = jnp.concatenate([orecv[b, src, core, g] for src in range(4) for core in range(2) for g in range(2)], axis=1)
        attn = jnp.dot(lhs, jnp.concatenate([wo[src] for src in range(4)], axis=0), preferred_element_type=F32)
        for hf in range(2):
            at = slice(cols[hf], cols[hf] + 512)
            mlp_tot = mpart[y, hf, b].astype(F32) + mrs1[hf, 0, b].astype(F32) + mrs2[hf, b].astype(F32)
            out[own_rows, at] = (hid[own_rows, at].astype(F32) + attn[:, at] + mlp_tot).astype(BF16)
            ag1_copy(b, hf).start()
        for hf in range(2):
            ag2_copy(b, hf, 0).start()

    def early_sends():
        for cpy in caches:
            cpy.wait()
        for i in range(4):
            @pl.when(x == i)
            def _():
                bytes_of(kvbuf.at[pl.ds(0, (5, 4, 3, 1)[i])], kvs_sem.at[0], kvr_sem.at[0]).wait_send()

        bytes_of(kvbuf.at[pl.ds(0, 2)], dds_sem.at[0], ddr_sem.at[0]).wait_send()
        bytes_of(kvbuf.at[pl.ds(0, 9)], es_sem.at[0], er_sem.at[0]).wait_send()

    def step3(b):
        @pl.when(b == blocks - 1)
        def _():
            early_sends()

        for hf in range(2):
            ag1_wait(b, hf)
            ag2_copy(b, hf, 1).start()

    def out_copy(b):
        return pltpu.make_async_copy(out.at[block_rows(b)], out_hbm.at[block_rows(b)], out_sem.at[0])

    def step4(b):
        bytes_of(hid.at[pl.ds(0, 2 * quarter)], ys_sem.at[b], yr_sem.at[b, 4]).wait_recv()
        out_copy(b).start()

    n = 2 * x

    def chunk_of(s):
        first_half = s // 2
        par = s % 2
        near = 2 * (x - 1 - first_half) + (c + par - 2 * c * par)
        mix_half = c + first_half - 2 * c * first_half
        mixed = 4 - 4 * par + mix_half
        late = 2 + (c + par - 2 * c * par)
        three = jnp.where(s < 4, mixed, late)
        return jnp.where(x == 3, three, near)

    three = x == 3
    lead = 2 * (x // 2) + x // 3
    ticks = lead + 8 + 2 * (x // 3)

    def pick(tau, near, far):
        b = jnp.int32(-1)
        for i in range(4):
            b = jnp.where(tau == jnp.where(three, far[i], near[i]), i, b)
        return jnp.maximum(b, 0), b >= 0

    def loop(t, carry):
        tau = t - lead
        gap = jnp.logical_and(three, jnp.logical_or(tau == 0, tau == 3))
        s = jnp.where(t == 2, 2, 0)
        pair = jnp.where(t == 1, 1, 0)

        @pl.when(jnp.logical_and(tau < 0, t != 1))
        def _():
            ch_b = chunk_of(s + 1)
            kv_copy(ch_b, 0, right).wait_recv()

            @pl.when(jnp.logical_and(three, t == 0))
            def _():
                kv_copy(ch_b, 0, left).start()

            @pl.when(x == 2)
            def _():
                kv_copy(ch_b, 1, right).start()

            kv_copy(chunk_of(s), 0, right).wait_recv()

        @pl.when(jnp.logical_and(x > 0, tau == x // 3))
        def _():
            kv_copy(chunk_of(n - 2), 0, right).wait_recv()
            kv_copy(chunk_of(n - 1), 0, right).wait_recv()

            @pl.when(x == 1)
            def _():
                kv_copy(chunk_of(1), 3, right).start()

        @pl.when(t == (x // 2) * (x - 1))
        def _():
            with jax.named_scope('e2'):
                for hf in range(2):
                    mlp_rs1(hf, 1).wait_recv()
                    msum[hf] = (mpart[second[hf], hf].astype(F32) + mrs1[hf, 1].astype(F32)).astype(BF16)
                    mlp_rs2(hf).start()

        @pl.when(tau == x // 3)
        def _():
            with jax.named_scope('e3'):
                bytes_of(wo.at[far, pl.ds(0, w_half)], es_sem.at[0], er_sem.at[2]).wait_recv()
                for i in range(3):
                    wo_partner(i).start()

        @pl.when(tau < 0)
        def _():
            with jax.named_scope('att'):
                attend_pair(chunk_of(s), chunk_of(s + 1), pair)

        b0, ok0 = pick(tau, (0, 1, 2, 3), (1, 2, 4, 5))

        @pl.when(jnp.logical_and(jnp.logical_or(ok0, gap), x > 0))
        def _():
            back = jnp.where(gap, 4, 2)
            with jax.named_scope('last'):
                attend_last(chunk_of(n - back), chunk_of(n - back + 1), jnp.where(gap, 2 + tau // 3, b0))

        def service(fn, nm, near_t, far_t):
            bk, okk = pick(tau, near_t, far_t)

            @pl.when(okk)
            def _():
                with jax.named_scope(nm):
                    fn(bk)

        service(step3, 's3', (4, 5, 6, 7), (5, 6, 8, 9))
        service(step1, 's1', (1, 2, 3, 4), (2, 3, 5, 6))

        @pl.when(ok0)
        def _():
            with jax.named_scope('finish'):
                finish(b0)

        service(step2, 's2', (2, 3, 4, 5), (3, 4, 5, 7))
        return carry

    lax.fori_loop(0, ticks, loop, 0)

    def last_step(b, carry):
        with jax.named_scope('s4'):
            step4(b)
        return carry

    lax.fori_loop(0, blocks, last_step, 0)

    for b in range(blocks):
        pieces = 7 + 12 + (2 if b < straight else 0)
        bytes_of(hid.at[pl.ds(0, pieces * quarter // 4)], ys_sem.at[b], yr_sem.at[b, 0]).wait_send()
    pltpu.make_async_copy(out, out_hbm, out_sem.at[0]).wait()


def layer(hidden, positions, gain, w_q, w_k, w_v, w_gate, w_up, w_down, w_o):
    rows, width = hidden.shape
    ff = w_gate.shape[1]
    hr = 256
    nb = rows // hr
    qr = hr // 4
    hw = width // 2
    freq = 1.0 / (ROPE_BASE ** (np.repeat(np.arange(0, HEAD_DIM, 2), 2) / HEAD_DIM))
    freq = jnp.asarray(freq[None, :], F32)
    anyspec = pl.BlockSpec(memory_space=pl.ANY)
    vm = pltpu.VMEM
    dma = pltpu.SemaphoreType.DMA
    return pl.pallas_call(
        layer_kernel,
        in_specs=[anyspec] * 11,
        out_specs=[anyspec] * 3,
        out_shape=[jax.ShapeDtypeStruct((rows, width), BF16),
                   jax.ShapeDtypeStruct((rows * w_k.shape[1] // HEAD_DIM, HEAD_DIM), BF16),
                   jax.ShapeDtypeStruct((rows * w_v.shape[1] // HEAD_DIM, HEAD_DIM), BF16)],
        scratch_shapes=[
            vm((9, 2, rows, HEAD_DIM), BF16),
            vm((3, 2, rows, HEAD_DIM), BF16),
            vm((2, 2, rows, HEAD_DIM), F32),
            vm((2, 2, rows, HEAD_DIM), F32),
            vm((2, 2, rows, HEAD_DIM), F32),
            vm((rows, width), BF16),
            vm((rows, width), BF16),
            vm((rows // HEAD_DIM, HEAD_DIM), jnp.int32),
            vm((width // HEAD_DIM, HEAD_DIM), BF16),
            vm((1, HEAD_DIM), F32),
            vm((rows, HEAD_DIM), F32),
            vm((rows, HEAD_DIM), F32),
            vm(w_q.shape, BF16), vm(w_k.shape, BF16), vm(w_v.shape, BF16),
            vm((width, ff), BF16), vm((width, ff), BF16), vm((ff, width), BF16),
            vm((4,) + w_o.shape, BF16),
            vm((2, 2 * hr, HEAD_DIM), F32),
            vm((rows * w_k.shape[1] // HEAD_DIM, HEAD_DIM), BF16),
            vm((rows * w_v.shape[1] // HEAD_DIM, HEAD_DIM), BF16),
            vm((4, 2, nb, qr, hw), BF16),
            vm((2, 2, nb, qr, hw), BF16),
            vm((2, nb, qr, hw), BF16),
            vm((2, nb, qr, hw), BF16),
            vm((nb, 4, 2, 2, qr, HEAD_DIM), BF16),
            vm((nb, 4, 2, 2, qr, HEAD_DIM), BF16),
            vm((nb, 2, 2, qr, HEAD_DIM), BF16),
            vm((rows, width), BF16),
            dma((13,)), dma((nb,)), dma((1,)), dma((8,)), dma((1,)), dma((2,)), dma((1,)), dma((8,)),
            dma((nb,)), dma((nb, 5)), dma((1,)),
        ],
        compiler_params=pltpu.CompilerParams(collective_id=0, has_side_effects=True, vmem_limit_bytes=62 << 20),
        name='layer',
    )(hidden, positions.reshape(rows // HEAD_DIM, HEAD_DIM), gain.reshape(width // HEAD_DIM, HEAD_DIM), freq,
      w_q, w_k, w_v, w_gate, w_up, w_down, w_o)


def solution(mesh):
    def local_layer(hidden, positions, ln_gain, w_q, w_k, w_v, w_o, w_gate, w_up, w_down):
        rows = hidden.shape[0]
        kv_local = w_k.shape[1] // HEAD_DIM
        out, kc, vc = layer(hidden, positions, ln_gain, w_q, w_k, w_v, w_gate, w_up, w_down, w_o)
        return out, kc.reshape(rows, kv_local, HEAD_DIM), vc.reshape(rows, kv_local, HEAD_DIM)

    row_spec = P(('dp', 'cp'), None)
    col_spec = P(None, 'tp')
    cache_spec = P(('dp', 'cp'), 'tp', None)
    in_specs = (row_spec, P(('dp', 'cp')), P(None), col_spec, col_spec, col_spec, P('tp', None), col_spec, col_spec, P('tp', None))
    return jax.shard_map(local_layer, mesh=mesh, in_specs=in_specs, out_specs=(row_spec, cache_spec, cache_spec), check_vma=False)
```
